32 devices in a mesh: dp: 4 (over z), replica: 2 (over y), fsdp: 4 (over x, core).
Axes of the slice: x: 2, y: 2, z: 4, core: 2. Of those that a mesh axis runs over, the one named last changes fastest.
Arguments:
- x_tokens: bfloat16 [131072, 768], P(('dp', 'replica', 'fsdp'))
- dy_tokens: bfloat16 [131072, 768], P(('dp', 'replica', 'fsdp'))
- w_gate: bfloat16 [2, 768, 3072], P(None, 'fsdp')
- w_up: bfloat16 [2, 768, 3072], P(None, 'fsdp')
- w_down: bfloat16 [2, 3072, 768], P(None, 'fsdp')
- norm_gain: float32 [2, 768], replicated
Outputs:
- output 1: bfloat16 [131072, 768], P(('dp', 'replica', 'fsdp'))
- output 2: float32 [2, 768, 3072], P(None, 'fsdp')
- output 3: float32 [2, 768, 3072], P(None, 'fsdp')
- output 4: float32 [2, 3072, 768], P(None, 'fsdp')
- output 5: float32 [2, 768], replicated
All inputs are finite; a program needn't handle non-finite values.
Results may differ from the reference program's by a relative error of at most 0.0148433.
Values are sent between devices in bfloat16 or wider.
A program may use at most 1 GiB of HBM per device.

```python
import jax
import jax.numpy as jnp
from jax import lax

D = 768
FF = 3072
LAYERS = 2
BLOCK_TOK = 4096
N_BLOCKS = 32
NORM_EPS = 1e-6
TOKENS = BLOCK_TOK * N_BLOCKS


def setup_inputs(seed: int = 0) -> dict:
    root_key = jax.random.key(seed)
    subkeys = jax.random.split(root_key, 6)
    in_scale = D ** -0.5
    inner_scale = FF ** -0.5
    x_tokens = jax.random.normal(subkeys[0], (TOKENS, D), jnp.float32).astype(jnp.bfloat16)
    dy_tokens = jax.random.normal(subkeys[1], (TOKENS, D), jnp.float32).astype(jnp.bfloat16)
    w_gate = (jax.random.normal(subkeys[2], (LAYERS, D, FF), jnp.float32) * in_scale).astype(jnp.bfloat16)
    w_up = (jax.random.normal(subkeys[3], (LAYERS, D, FF), jnp.float32) * in_scale).astype(jnp.bfloat16)
    w_down = (jax.random.normal(subkeys[4], (LAYERS, FF, D), jnp.float32) * inner_scale).astype(jnp.bfloat16)
    norm_gain = jax.random.uniform(subkeys[5], (LAYERS, D), jnp.float32, 0.5, 1.5)
    return {"x_tokens": x_tokens, "dy_tokens": dy_tokens, "w_gate": w_gate, "w_up": w_up, "w_down": w_down, "norm_gain": norm_gain}


def snap_bf16(values):
    return values.astype(jnp.bfloat16).astype(jnp.float32)


def layer_apply(hidden, layer_params):
    w_gate, w_up, w_down, gain_row = layer_params
    inv_rms = lax.rsqrt(jnp.mean(hidden * hidden, axis=-1, keepdims=True) + NORM_EPS)
    normed = snap_bf16(hidden * inv_rms * gain_row)
    gate_act = snap_bf16(jnp.dot(normed, w_gate, preferred_element_type=jnp.float32))
    up_act = snap_bf16(jnp.dot(normed, w_up, preferred_element_type=jnp.float32))
    prod_act = snap_bf16(jax.nn.silu(gate_act) * up_act)
    layer_out = snap_bf16(hidden + jnp.dot(prod_act, w_down, preferred_element_type=jnp.float32))
    return layer_out, None


def stack_apply(params, x_block):
    return lax.scan(layer_apply, x_block, params)[0]


def reference(x_tokens, dy_tokens, w_gate, w_up, w_down, norm_gain):
    params = (w_gate.astype(jnp.float32), w_up.astype(jnp.float32), w_down.astype(jnp.float32), norm_gain)
    x_blocks = x_tokens.reshape(N_BLOCKS, BLOCK_TOK, D)
    dy_blocks = dy_tokens.reshape(N_BLOCKS, BLOCK_TOK, D)

    def block_step(grad_sum, block_pair):
        x_block = block_pair[0].astype(jnp.float32)
        dy_block = block_pair[1].astype(jnp.float32)
        y_block, pull_back = jax.vjp(lambda weights: stack_apply(weights, x_block), params)
        block_grads = pull_back(dy_block)[0]
        return jax.tree.map(jnp.add, grad_sum, block_grads), y_block.astype(jnp.bfloat16)

    grad_zero = jax.tree.map(jnp.zeros_like, params)
    grad_sum, y_blocks = lax.scan(block_step, grad_zero, (x_blocks, dy_blocks))
    y_tokens = y_blocks.reshape(TOKENS, D)
    return (y_tokens, grad_sum[0], grad_sum[1], grad_sum[2], grad_sum[3])
```

```python
import jax
import jax.numpy as jnp
from jax import lax
from jax.experimental import pallas as pl
from jax.experimental.pallas import tpu as pltpu
from jax.sharding import PartitionSpec as P

NORM_EPS = 1e-6
TOKEN_AXES = ("dp", "replica", "fsdp")
MESH_ID = pl.DeviceIdType.MESH
BF16 = jnp.bfloat16
F32 = jnp.float32

TOK = 4096
D = 768
FF = 3072
LAYERS = 2
TM = 512
NT = TOK // TM
FT = 512
NF = FF // FT
GR = D // 4
UNITS = LAYERS * NF
TILES = LAYERS * NF
JOBS = 3 * TILES
BLK = (384, 256)
VMEM_MAX = 67043328
O1, O2, O3, O4, O5, O6, O7 = 1, 3, 4, 5, 6, 7, 8
TICKS = JOBS + O7
MAIN = LAYERS * NF * NT
DRAIN = TICKS - 3 * (TILES - 1)


def dot_nn(a, b):
    return lax.dot_general(a, b, (((1,), (0,)), ((), ())), preferred_element_type=F32)


def dot_nt(a, b):
    return lax.dot_general(a, b, (((1,), (1,)), ((), ())), preferred_element_type=F32)


def dot_tn(a, b):
    return lax.dot_general(a, b, (((0,), (0,)), ((), ())), preferred_element_type=F32)


def sigmoid(v):
    return 0.5 * jnp.tanh(0.5 * v) + 0.5


def inv_rms_of(h):
    return lax.rsqrt(jnp.mean(h * h, axis=-1, keepdims=True) + NORM_EPS)


def rows_of(start, size, unit):
    return pl.ds(pl.multiple_of(start, unit), size)


def place():
    shard = lax.axis_index("fsdp")
    return shard, shard // 2, shard % 2, lax.axis_index("replica"), lax.axis_index("dp")


def entry_barrier(partners):
    barrier = pltpu.get_barrier_semaphore()
    for partner in partners:
        pl.semaphore_signal(barrier, inc=1, device_id=partner, device_id_type=MESH_ID)
    pl.semaphore_wait(barrier, len(partners))


def gather_kernel(x_blk, gain_blk, wg_sh, wu_sh, wd_sh, gu_out, h1_out, wgu_hbm, wd_hbm,
                  n_all, acc, wgu, wd, load_sem, send_sem, recv_sem, out_sem):
    step = pl.program_id(0)
    tile = step // NT
    tok = step % NT
    shard, xx, cc, yy, zz = place()
    core_dev = {"fsdp": 2 * xx + (1 - cc)}
    x_dev = {"fsdp": 2 * (1 - xx) + cc}
    y_dev = {"replica": 1 - yy}
    core_sh = 2 * xx + (1 - cc)
    x_sh = 2 * (1 - xx) + cc
    far_sh = 2 * (1 - xx) + (1 - cc)

    def part(unit, owner, half):
        if half is None:
            return wgu.at[unit, rows_of(owner * GR, GR, GR), :], wd.at[unit, rows_of(owner * 128, 128, 128), :]
        return (wgu.at[unit, rows_of(owner * GR + half * 96, 96, 96), :],
                wd.at[unit, rows_of(owner * 128 + half * 64, 64, 64), :])

    def message(unit, kind, owner, half, dev):
        return [pltpu.make_async_remote_copy(src_ref=ref, dst_ref=ref, send_sem=send_sem.at[unit, kind, i],
                                             recv_sem=recv_sem.at[unit, kind, i], device_id=dev,
                                             device_id_type=MESH_ID)
                for i, ref in enumerate(part(unit, owner, half))]

    def send(unit, kind, owner, half, dev):
        for copy in message(unit, kind, owner, half, dev):
            copy.start()

    def arrived(unit, kind, owner, half, dev):
        for copy in message(unit, kind, owner, half, dev):
            copy.wait_recv()

    def load(unit):
        layer = unit // NF
        col = (unit % NF) * 128
        for group in range(4):
            cols = rows_of(group * D + col, 128, 128)
            pltpu.make_async_copy(wg_sh.at[layer, :, cols],
                                  wgu.at[unit, rows_of(shard * GR, GR, GR), pl.ds(group * 128, 128)],
                                  load_sem.at[unit, 0]).start()
            pltpu.make_async_copy(wu_sh.at[layer, :, cols],
                                  wgu.at[unit, rows_of(shard * GR, GR, GR), pl.ds(FT + group * 128, 128)],
                                  load_sem.at[unit, 0]).start()
        pltpu.make_async_copy(wd_sh.at[layer, rows_of(col, 128, 128), :],
                              wd.at[unit, rows_of(shard * 128, 128, 128), :], load_sem.at[unit, 1]).start()

    def send_own(unit):
        own = part(unit, shard, None)
        for i in range(2):
            pltpu.make_async_copy(own[i], own[i], load_sem.at[unit, i]).wait()
        send(unit, 1, shard, yy, x_dev)
        send(unit, 0, shard, None, core_dev)

    def forward_x(unit):
        arrived(unit, 1, x_sh, yy, x_dev)
        send(unit, 2, x_sh, yy, y_dev)
        send(unit, 3, x_sh, yy, core_dev)

    def forward_y(unit):
        arrived(unit, 2, x_sh, 1 - yy, y_dev)
        send(unit, 4, x_sh, 1 - yy, core_dev)

    def outs(unit):
        return (pltpu.make_async_copy(wgu.at[unit], wgu_hbm.at[unit], out_sem.at[unit, 0]),
                pltpu.make_async_copy(wd.at[unit], wd_hbm.at[unit], out_sem.at[unit, 1]))

    def complete(unit):
        arrived(unit, 0, core_sh, None, core_dev)
        arrived(unit, 3, far_sh, yy, core_dev)
        arrived(unit, 4, far_sh, 1 - yy, core_dev)
        for copy in outs(unit):
            copy.start()

    @pl.when(step == 0)
    def _():
        @pl.loop(0, UNITS)
        def _(unit):
            load(unit)

        entry_barrier((core_dev, x_dev, y_dev))

        @pl.loop(0, 4)
        def _(unit):
            send_own(unit)

        forward_x(0)
        forward_y(0)

    @pl.when(jnp.logical_and(step % 4 == 1, step // 4 + 1 < UNITS))
    def _():
        unit = step // 4 + 1

        @pl.when(unit + 3 < UNITS)
        def _():
            send_own(unit + 3)

        forward_x(unit)

    @pl.when(jnp.logical_and(step % 4 == 0, step >= 4))
    def _():
        forward_y(step // 4)

    @pl.when(tok == 0)
    def _():
        complete(tile)

    @pl.when(jnp.logical_and(step % 4 == 3, step // 4 >= NF))
    def _():
        complete(step // 4)

    rows = rows_of(tok * TM, TM, TM)

    @pl.when(tile == 0)
    def _():
        h = x_blk[...].astype(F32)
        n_all[rows, :] = (h * inv_rms_of(h) * gain_blk[0:1, :]).astype(BF16)

    gu = dot_nn(n_all[rows, :], wgu[tile]).astype(BF16)
    gu_out[0] = gu
    gate = gu[:, :FT].astype(F32)
    prod = (gate * sigmoid(gate) * gu[:, FT:].astype(F32)).astype(BF16)
    acc[rows, :] = jnp.where(tile == 0, 0.0, acc[rows, :]) + dot_nn(prod, wd[tile])

    @pl.when(tile == NF - 1)
    def _():
        h1_out[...] = (x_blk[...].astype(F32) + acc[rows, :]).astype(BF16)

    @pl.when(step == NF * NT - 1)
    def _():
        @pl.loop(0, UNITS)
        def _(unit):
            for kind, owner, half, dev in ((0, shard, None, core_dev), (1, shard, yy, x_dev), (2, x_sh, yy, y_dev),
                                           (3, x_sh, yy, core_dev), (4, x_sh, 1 - yy, core_dev)):
                for copy in message(unit, kind, owner, half, dev):
                    copy.wait_send()
            for copy in outs(unit):
                copy.wait()


def forward_gather(x, gain, wg_sh, wu_sh, wd_sh):
    any_spec = pl.BlockSpec(memory_space=pl.ANY)

    def x_index(s):
        return (jnp.where(jnp.logical_or(s // NT == 0, s // NT == NF - 1), s % NT, NT - 1), 0)

    return pl.pallas_call(
        gather_kernel,
        grid=(NF * NT,),
        in_specs=[pl.BlockSpec((TM, D), x_index), pl.BlockSpec((LAYERS, D), lambda s: (0, 0)),
                  any_spec, any_spec, any_spec],
        out_specs=[pl.BlockSpec((1, TM, 2 * FT), lambda s: (s // NT, s % NT, 0)),
                   pl.BlockSpec((TM, D), lambda s: (jnp.where(s // NT == NF - 1, s % NT, 0), 0)),
                   any_spec, any_spec],
        out_shape=[jax.ShapeDtypeStruct((NF, TOK, 2 * FT), BF16), jax.ShapeDtypeStruct((TOK, D), BF16),
                   jax.ShapeDtypeStruct((UNITS, D, 2 * FT), BF16), jax.ShapeDtypeStruct((UNITS, FT, D), BF16)],
        scratch_shapes=[pltpu.VMEM((TOK, D), BF16), pltpu.VMEM((TOK, D), F32),
                        pltpu.VMEM((UNITS, D, 2 * FT), BF16), pltpu.VMEM((UNITS, FT, D), BF16),
                        pltpu.SemaphoreType.DMA((UNITS, 2)), pltpu.SemaphoreType.DMA((UNITS, 5, 2)),
                        pltpu.SemaphoreType.DMA((UNITS, 5, 2)), pltpu.SemaphoreType.DMA((UNITS, 2))],
        compiler_params=pltpu.CompilerParams(collective_id=1, has_side_effects=True, vmem_limit_bytes=VMEM_MAX),
        cost_estimate=pl.CostEstimate(flops=6 * TOK * D * FF, bytes_accessed=100 << 20, transcendentals=0),
        name="forward_gather",
    )(x, gain, wg_sh, wu_sh, wd_sh)


def grads_kernel(h1_blk, x_blk, gain_blk, wgu_blk, wd_blk, gu_blk, dy_hbm, prod_out, parts, fin, gain_out,
                 n_all, cot_all, dn_all, acc_gu, acc_d, gain_acc, own, r_core, sum_c, r_x, sum_x, r_y, sum_y, r_z, done,
                 g_recv, g_zrecv, cot_sem, part_sem, own_sem, core_send, core_recv, x_send, x_recv, y_send, y_recv,
                 z_send, z_recv, dz_send, dz_recv, dy_send, dy_recv, fin_sem, gs_send, gs_recv, gz_send, gz_recv):
    step = pl.program_id(0)
    wide = step // NT
    tok = step % NT
    layer0 = step >= NF * NT
    tile = wide % NF
    slot = wide % 2
    shard, xx, cc, yy, zz = place()
    core_dev = {"fsdp": 2 * xx + (1 - cc)}
    x_dev = {"fsdp": 2 * (1 - xx) + cc}
    y_dev = {"replica": 1 - yy}
    z_devs = [{"dp": (zz + k) % 4} for k in (1, 2, 3)]

    def remote(src, dst, send, recv, dev):
        return pltpu.make_async_remote_copy(src_ref=src, dst_ref=dst, send_sem=send, recv_sem=recv, device_id=dev,
                                            device_id_type=MESH_ID)

    half_mine = rows_of(yy * 192, 192, 192)
    half_other = rows_of((1 - yy) * 192, 192, 192)

    def core_copy(j):
        return remote(parts.at[j, 1 - cc], r_core.at[j % 2], core_send, core_recv.at[j % 2], core_dev)

    def own_copy(j):
        return pltpu.make_async_copy(parts.at[j, cc], own, own_sem)

    def x_copy(j):
        return remote(sum_c.at[j % 2, 1 - xx], r_x.at[j % 4], x_send.at[j % 2], x_recv.at[j % 4], x_dev)

    def y_copy(j):
        return remote(sum_x.at[half_other, :], r_y.at[j % 2], y_send, y_recv.at[j % 2], y_dev)

    def z_copies(j):
        return [remote(sum_y.at[rows_of(((zz + k + 1) % 4) * 48, 48, 48), :], r_z.at[j % 2, k], z_send.at[k],
                       z_recv.at[j % 2, k], dev) for k, dev in enumerate(z_devs)]

    def quarter(q):
        return rows_of(yy * 192 + q * 48, 48, 48)

    def done_z_copies(j):
        ref = done.at[j % 4, quarter(zz), :]
        return [remote(ref, ref, dz_send.at[k], dz_recv.at[j % 2, k], dev) for k, dev in enumerate(z_devs)]

    def done_y_copy(j):
        ref = done.at[j % 4, half_mine, :]
        return remote(ref, ref, dy_send, dy_recv.at[j % 2], y_dev)

    def fin_copy(j):
        return pltpu.make_async_copy(done.at[j % 4], fin.at[j], fin_sem.at[j % 2])

    def stage0(j):
        whole = parts.at[j]
        pltpu.make_async_copy(whole, whole, part_sem.at[j % 3]).wait()
        own_copy(j).start()
        core_copy(j).start()

    def stage1(j):
        own_copy(j).wait()
        core_copy(j).wait()
        sum_c[j % 2] = own[...] + r_core[j % 2]
        x_copy(j).start()

    def stage2(j):
        x_copy(j).wait()
        sum_x[...] = sum_c[j % 2, xx] + r_x[j % 4]
        y_copy(j).start()

    def stage3(j):
        y_copy(j).wait()
        sum_y[...] = sum_x[half_mine, :] + r_y[j % 2]
        for copy in z_copies(j):
            copy.start()

    def stage4(j):
        for copy in z_copies(j):
            copy.wait()
        done[j % 4, quarter(zz), :] = (sum_y[rows_of(zz * 48, 48, 48), :] + r_z[j % 2, 0]) + (r_z[j % 2, 1] + r_z[j % 2, 2])
        for copy in done_z_copies(j):
            copy.start()

    def stage5(j):
        for copy in done_z_copies(j):
            copy.wait()
        done_y_copy(j).start()

    def stage6(j):
        done_y_copy(j).wait()
        fin_copy(j).start()

    def stage7(j):
        fin_copy(j).wait()

    def tick(count):
        for offset, stage in ((O7, stage7), (O6, stage6), (O5, stage5), (O4, stage4), (O3, stage3), (O2, stage2),
                              (O1, stage1), (0, stage0)):
            job = count - offset

            @pl.when(jnp.logical_and(job >= 0, job < JOBS))
            def _():
                stage(job)

    def write_parts(which, at):
        for s in range(4):
            for k in range(3):
                pltpu.make_async_copy(acc_d.at[at, pl.ds(s * 128, 128), pl.ds(k * 256, 256)],
                                      parts.at[3 * which, s % 2, s // 2, pl.ds(k * 128, 128), :],
                                      part_sem.at[0]).start()
            for m in range(2):
                for k in range(2):
                    pltpu.make_async_copy(acc_gu.at[at, pl.ds(s * GR, GR), pl.ds(m * FT + k * 256, 256)],
                                          parts.at[3 * which + 1 + m, s % 2, s // 2, pl.ds(k * 192, 192), :],
                                          part_sem.at[1 + m]).start()

    @pl.when(step == 0)
    def _():
        load = pltpu.make_async_copy(dy_hbm, cot_all, cot_sem)
        load.start()
        gain_acc[0] = jnp.zeros_like(gain_acc[0])
        entry_barrier((core_dev, x_dev, y_dev, *z_devs))
        load.wait()

    @pl.when(jnp.logical_and(tok == 0, jnp.logical_and(wide >= 1, wide <= TILES)))
    def _():
        write_parts(wide - 1, (wide - 1) % 2)

    in_main = step < MAIN

    @pl.when(jnp.logical_and(jnp.logical_and(in_main, wide >= 1), tok % 3 == 1))
    def _():
        tick(3 * (wide - 1) + tok // 3)

    rows = rows_of(tok * TM, TM, TM)
    first_tok = tok == 0
    first_tile = tile == 0

    def normed(h_ref, row):
        h = h_ref[...].astype(F32)
        n_all[rows, :] = (h * inv_rms_of(h) * gain_blk[row:row + 1, :]).astype(BF16)

    def backward(gu, prod_ref):
        cot = cot_all[rows, :]
        d_prod = dot_nt(cot, wd_blk[0]).astype(BF16).astype(F32)
        gate = gu[:, :FT].astype(F32)
        up = gu[:, FT:].astype(F32)
        sig = sigmoid(gate)
        silu = gate * sig
        prod = (silu * up).astype(BF16)
        if prod_ref is not None:
            prod_ref[0] = prod
        d_up = (d_prod * silu).astype(BF16)
        d_gate = ((d_prod * up) * (sig + silu * (1.0 - sig))).astype(BF16)
        d_gu = jnp.concatenate([d_gate, d_up], axis=1)
        acc_d[slot] = jnp.where(first_tok, 0.0, acc_d[slot]) + dot_tn(prod, cot)
        acc_gu[slot] = jnp.where(first_tok, 0.0, acc_gu[slot]) + dot_tn(n_all[rows, :], d_gu)
        dn_all[rows, :] = jnp.where(first_tile, 0.0, dn_all[rows, :]) + dot_nt(d_gu, wgu_blk[0])

    def norm_backward(h_ref, row, want_hidden):
        h = h_ref[...].astype(F32)
        inv = inv_rms_of(h)
        dn = dn_all[rows, :].astype(BF16).astype(F32)
        part = jnp.sum(dn * h * inv, axis=0, keepdims=True)
        gain_acc[0, row:row + 1, :] = jnp.where(first_tok, 0.0, gain_acc[0, row:row + 1, :]) + part
        if want_hidden:
            scaled = dn * gain_blk[row:row + 1, :]
            back = inv * scaled - h * (inv * inv * inv) * jnp.mean(scaled * h, axis=-1, keepdims=True)
            cot_all[rows, :] = (cot_all[rows, :].astype(F32) + back).astype(BF16)

    @pl.when(jnp.logical_not(layer0))
    def _():
        @pl.when(first_tile)
        def _():
            normed(h1_blk, 1)

        backward(dot_nn(n_all[rows, :], wgu_blk[0]).astype(BF16), prod_out)

        @pl.when(tile == NF - 1)
        def _():
            norm_backward(h1_blk, 1, True)

    @pl.when(jnp.logical_and(layer0, in_main))
    def _():
        @pl.when(first_tile)
        def _():
            normed(x_blk, 0)

        backward(gu_blk[0], None)

        @pl.when(tile == NF - 1)
        def _():
            norm_backward(x_blk, 0, False)

    def gain_copy(leg, dev):
        return remote(gain_acc.at[leg], g_recv.at[leg], gs_send.at[leg], gs_recv.at[leg], dev)

    def gain_z_copies():
        return [remote(g_zrecv.at[zz], g_zrecv.at[zz], gz_send.at[k], gz_recv.at[k], dev)
                for k, dev in enumerate(z_devs)]

    legs = (core_dev, x_dev, y_dev)

    @pl.when(jnp.logical_not(in_main))
    def _():
        tick(3 * (TILES - 1) + step - MAIN)

        for leg in range(4):
            @pl.when(step == MAIN + 1 + leg)
            def _():
                if leg > 0:
                    gain_copy(leg - 1, legs[leg - 1]).wait()
                    total = gain_acc[leg - 1] + g_recv[leg - 1]
                    if leg < 3:
                        gain_acc[leg] = total
                    else:
                        g_zrecv[zz] = total
                if leg < 3:
                    gain_copy(leg, legs[leg]).start()
                else:
                    for copy in gain_z_copies():
                        copy.start()

        @pl.when(step == MAIN + 6)
        def _():
            for copy in gain_z_copies():
                copy.wait()
            gain_out[...] = (g_zrecv[0] + g_zrecv[1]) + (g_zrecv[2] + g_zrecv[3])


def backward_reduce(h1, x, gain, wgu, wd, gu0, dy):
    any_spec = pl.BlockSpec(memory_space=pl.ANY)
    half = NF * NT

    def hold(s, base):
        r = jnp.clip(s - base, 0, half - 1)
        return (jnp.where(jnp.logical_or(r // NT == 0, r // NT == NF - 1), r % NT, NT - 1), 0)

    def unit_index(s):
        wide = jnp.minimum(s, MAIN - 1) // NT
        return (jnp.where(wide < NF, NF + wide, wide - NF), 0, 0)

    def gu_index(s):
        r = jnp.clip(s - half, 0, half - 1)
        return (r // NT, r % NT, 0)

    def prod_index(s):
        r = jnp.minimum(s, half - 1)
        return (r // NT, r % NT, 0)

    dma = pltpu.SemaphoreType.DMA
    return pl.pallas_call(
        grads_kernel,
        grid=(MAIN + DRAIN,),
        in_specs=[pl.BlockSpec((TM, D), lambda s: hold(s, 0)), pl.BlockSpec((TM, D), lambda s: hold(s, half)),
                  pl.BlockSpec((LAYERS, D), lambda s: (0, 0)), pl.BlockSpec((1, D, 2 * FT), unit_index),
                  pl.BlockSpec((1, FT, D), unit_index), pl.BlockSpec((1, TM, 2 * FT), gu_index), any_spec],
        out_specs=[pl.BlockSpec((1, TM, FT), prod_index), any_spec, any_spec,
                   pl.BlockSpec((8, D), lambda s: (0, 0))],
        out_shape=[jax.ShapeDtypeStruct((NF, TOK, FT), BF16), jax.ShapeDtypeStruct((JOBS, 2, 2, *BLK), F32),
                   jax.ShapeDtypeStruct((JOBS, *BLK), F32), jax.ShapeDtypeStruct((8, D), F32)],
        scratch_shapes=[pltpu.VMEM((TOK, D), BF16), pltpu.VMEM((TOK, D), BF16), pltpu.VMEM((TOK, D), F32),
                        pltpu.VMEM((2, D, 2 * FT), F32), pltpu.VMEM((2, FT, D), F32), pltpu.VMEM((3, 8, D), F32),
                        pltpu.VMEM((2, *BLK), F32), pltpu.VMEM((2, 2, *BLK), F32), pltpu.VMEM((2, 2, *BLK), F32),
                        pltpu.VMEM((4, *BLK), F32), pltpu.VMEM(BLK, F32), pltpu.VMEM((2, 192, 256), F32),
                        pltpu.VMEM((192, 256), F32), pltpu.VMEM((2, 3, 48, 256), F32), pltpu.VMEM((4, *BLK), F32),
                        pltpu.VMEM((3, 8, D), F32), pltpu.VMEM((4, 8, D), F32),
                        dma, dma((3,)), dma, dma, dma((2,)), dma((2,)), dma((4,)), dma, dma((2,)),
                        dma((3,)), dma((2, 3)), dma((3,)), dma((2, 3)), dma, dma((2,)), dma((2,)),
                        dma((3,)), dma((3,)), dma((3,)), dma((3,))],
        compiler_params=pltpu.CompilerParams(collective_id=2, has_side_effects=True, vmem_limit_bytes=VMEM_MAX),
        cost_estimate=pl.CostEstimate(flops=28 * TOK * D * FF, bytes_accessed=300 << 20, transcendentals=0),
        name="backward_reduce",
    )(h1, x, gain, wgu, wd, gu0, dy)


def output_kernel(h1_blk, prod_blk, wd_blk, fin, y_out, d_gate, d_up, d_down, stage, load_sem, store_sem):
    step = pl.program_id(0)

    def fin_load(at, i):
        return pltpu.make_async_copy(fin.at[6 * at + i], stage.at[at % 3, i], load_sem.at[at % 3, i])

    def fin_store(at, i):
        wide = 2 * at + i // 3
        layer = 1 - wide // NF
        col = (wide % NF) * 128
        src = stage.at[at % 3, i]
        sem = store_sem.at[at % 3, i]
        if i % 3 == 0:
            for k in range(3):
                pltpu.make_async_copy(src.at[pl.ds(k * 128, 128), :],
                                      d_down.at[layer, rows_of(col, 128, 128), pl.ds(k * 256, 256)], sem).start()
        else:
            dst = d_gate if i % 3 == 1 else d_up
            for k in range(2):
                for g in range(2):
                    pltpu.make_async_copy(src.at[pl.ds(k * GR, GR), pl.ds(g * 128, 128)],
                                          dst.at[layer, :, rows_of((2 * k + g) * D + col, 128, 128)], sem).start()

    def fin_stored(at, i):
        src = stage.at[at % 3, i]
        pltpu.make_async_copy(src, src, store_sem.at[at % 3, i]).wait()

    per = JOBS // 6

    @pl.when(step >= 2)
    def _():
        for i in range(6):
            fin_stored(step - 2, i)

    @pl.when(jnp.logical_and(step >= 1, step <= per))
    def _():
        for i in range(6):
            fin_load(step - 1, i).wait()
            fin_store(step - 1, i)

    @pl.when(step < per)
    def _():
        for i in range(6):
            fin_load(step, i).start()

    out = dot_nn(prod_blk[0], wd_blk[0])
    for f in range(1, NF):
        out = out + dot_nn(prod_blk[f], wd_blk[f])
    y_out[...] = (h1_blk[...].astype(F32) + out).astype(BF16)


def layer_output(h1, prod, wd, fin):
    any_spec = pl.BlockSpec(memory_space=pl.ANY)
    shard = jax.ShapeDtypeStruct((LAYERS, GR, FF), F32)
    return pl.pallas_call(
        output_kernel,
        grid=(NT,),
        in_specs=[pl.BlockSpec((TM, D), lambda t: (t, 0)), pl.BlockSpec((NF, TM, FT), lambda t: (0, t, 0)),
                  pl.BlockSpec((NF, FT, D), lambda t: (1, 0, 0)), any_spec],
        out_specs=[pl.BlockSpec((TM, D), lambda t: (t, 0)), any_spec, any_spec, any_spec],
        out_shape=[jax.ShapeDtypeStruct((TOK, D), BF16), shard, shard, jax.ShapeDtypeStruct((LAYERS, D, D), F32)],
        scratch_shapes=[pltpu.VMEM((3, 6, *BLK), F32), pltpu.SemaphoreType.DMA((3, 6)), pltpu.SemaphoreType.DMA((3, 6))],
        compiler_params=pltpu.CompilerParams(vmem_limit_bytes=VMEM_MAX),
        cost_estimate=pl.CostEstimate(flops=2 * TOK * D * FF, bytes_accessed=72 << 20, transcendentals=0),
        name="layer_output",
    )(h1, prod, wd, fin)


def solution(mesh):
    tok_spec = P(TOKEN_AXES, None)
    shard_spec = P(None, "fsdp", None)
    full_spec = P(None, None)

    def device_step(x_local, dy_local, w_gate_sh, w_up_sh, w_down_sh, norm_gain):
        gu0, h1, wgu, wd = forward_gather(x_local, norm_gain, w_gate_sh, w_up_sh, w_down_sh)
        prod1, _, fin, gain_sum = backward_reduce(h1, x_local, norm_gain, wgu, wd, gu0, dy_local)
        y_local, d_gate, d_up, d_down = layer_output(h1, prod1, wd, fin)
        return y_local, d_gate, d_up, d_down, gain_sum[:LAYERS]

    return jax.shard_map(device_step, mesh=mesh,
                         in_specs=(tok_spec, tok_spec, shard_spec, shard_spec, shard_spec, full_spec),
                         out_specs=(tok_spec, shard_spec, shard_spec, shard_spec, full_spec), check_vma=False)
```

```python
import jax
import jax.numpy as jnp
from jax import lax
from jax.experimental import pallas as pl
from jax.experimental.pallas import tpu as pltpu
from jax.sharding import PartitionSpec as P

NORM_EPS = 1e-6
TOKEN_AXES = ("dp", "replica", "fsdp")
MESH_ID = pl.DeviceIdType.MESH
BF16 = jnp.bfloat16
F32 = jnp.float32

TOK = 4096
D = 768
FF = 3072
LAYERS = 2
TM = 512
NT = TOK // TM
FT = 512
NF = FF // FT
GR = D // 4
UNITS = LAYERS * NF
TILES = LAYERS * NF
JOBS = 3 * TILES
BLK = (384, 256)
VMEM_MAX = 67043328
O1, O2, O3, O4, O5, O6, O7 = 1, 4, 6, 9, 13, 17, 18
BEATS = 2 * (JOBS - 1) + O7 + 1
MAIN = LAYERS * NF * NT
STEPS = MAIN + NF * NT
AHEAD = 6
SLOW = 36


def dot_nn(a, b):
    return lax.dot_general(a, b, (((1,), (0,)), ((), ())), preferred_element_type=F32)


def dot_nt(a, b):
    return lax.dot_general(a, b, (((1,), (1,)), ((), ())), preferred_element_type=F32)


def dot_tn(a, b):
    return lax.dot_general(a, b, (((0,), (0,)), ((), ())), preferred_element_type=F32)


def sigmoid(v):
    return 0.5 * jnp.tanh(0.5 * v) + 0.5


def inv_rms_of(h):
    return lax.rsqrt(jnp.mean(h * h, axis=-1, keepdims=True) + NORM_EPS)


def rows_of(start, size):
    return pl.ds(pl.multiple_of(start, size), size)


def place():
    shard = lax.axis_index("fsdp")
    return shard, shard // 2, shard % 2, lax.axis_index("replica"), lax.axis_index("dp")


def signal_entry(partners):
    for partner in partners:
        pl.semaphore_signal(pltpu.get_barrier_semaphore(), inc=1, device_id=partner, device_id_type=MESH_ID)


def wait_entry(partners):
    pl.semaphore_wait(pltpu.get_barrier_semaphore(), len(partners))


def gather_kernel(x_hbm, gain_hbm, wg_sh, wu_sh, wd_sh, gu_hbm, h1_hbm, wgu_hbm, wd_hbm,
                  n_all, acc, prods, wgu, wd, x_buf, gu_buf, h1_buf, gain, load_sem, send_sem, recv_sem, out_sem,
                  x_sem, gu_sem, h1_sem, in_sem):
    step = pl.program_id(0)
    last = NF * NT - 1
    tile = jnp.minimum(step, last) >> 3
    tok = step & 7
    prev = jnp.maximum(step - 1, 0)
    prev_tile = prev >> 3
    side = step & 1
    shard, xx, cc, yy, zz = place()
    core_dev = {"fsdp": 2 * xx + (1 - cc)}
    x_dev = {"fsdp": 2 * (1 - xx) + cc}
    y_dev = {"replica": 1 - yy}
    core_sh = 2 * xx + (1 - cc)
    x_sh = 2 * (1 - xx) + cc
    far_sh = 2 * (1 - xx) + (1 - cc)
    both = (0, 1)

    def part(unit, owner, half):
        if half is None:
            return wgu.at[unit, rows_of(owner * GR, GR), :], wd.at[unit, rows_of(owner * 128, 128), :]
        return (wgu.at[unit, rows_of(owner * GR + half * 96, 96), :],
                wd.at[unit, rows_of(owner * 128 + half * 64, 64), :])

    def message(unit, kind, owner, half, dev, which=both):
        refs = part(unit, owner, half)
        return [pltpu.make_async_remote_copy(src_ref=refs[i], dst_ref=refs[i], send_sem=send_sem.at[kind, i],
                                             recv_sem=recv_sem.at[unit, kind, i], device_id=dev,
                                             device_id_type=MESH_ID)
                for i in which]

    def send(*args):
        for copy in message(*args):
            copy.start()

    def arrived(*args):
        for copy in message(*args):
            copy.wait_recv()

    def load(unit):
        layer = lax.div(unit, NF)
        col = lax.rem(unit, NF) * 128
        for group in range(4):
            cols = rows_of(group * D + col, 128)
            pltpu.make_async_copy(wg_sh.at[layer, :, cols],
                                  wgu.at[unit, rows_of(shard * GR, GR), pl.ds(group * 128, 128)],
                                  load_sem.at[unit, 0]).start()
            pltpu.make_async_copy(wu_sh.at[layer, :, cols],
                                  wgu.at[unit, rows_of(shard * GR, GR), pl.ds(FT + group * 128, 128)],
                                  load_sem.at[unit, 0]).start()
        pltpu.make_async_copy(wd_sh.at[layer, rows_of(col, 128), :],
                              wd.at[unit, rows_of(shard * 128, 128), :], load_sem.at[unit, 1]).start()

    def send_own(unit):
        own = part(unit, shard, None)
        for i in both:
            pltpu.make_async_copy(own[i], own[i], load_sem.at[unit, i]).wait()
            send(unit, 1, shard, yy, x_dev, (i,))
            send(unit, 0, shard, None, core_dev, (i,))

    def forward_x(unit, which=both):
        for i in which:
            arrived(unit, 1, x_sh, yy, x_dev, (i,))
            send(unit, 2, x_sh, yy, y_dev, (i,))
            send(unit, 3, x_sh, yy, core_dev, (i,))

    def forward_y(unit, which=both):
        for i in which:
            arrived(unit, 2, x_sh, 1 - yy, y_dev, (i,))
            send(unit, 4, x_sh, 1 - yy, core_dev, (i,))

    def out_copy(unit, i):
        if i == 0:
            return pltpu.make_async_copy(wgu.at[unit], wgu_hbm.at[unit], out_sem.at[0])
        return pltpu.make_async_copy(wd.at[unit], wd_hbm.at[unit], out_sem.at[1])

    def complete(unit, which=both):
        for i in which:
            arrived(unit, 0, core_sh, None, core_dev, (i,))
            arrived(unit, 3, far_sh, yy, core_dev, (i,))
            arrived(unit, 4, far_sh, 1 - yy, core_dev, (i,))
            out_copy(unit, i).start()

    def token_rows(at):
        return rows_of((at & 7) * TM, TM)

    def x_copy(at):
        return pltpu.make_async_copy(x_hbm.at[token_rows(at - 1), :], x_buf.at[at & 1], x_sem.at[at & 1])

    def gu_copy(at):
        return pltpu.make_async_copy(gu_buf.at[at & 1], gu_hbm.at[at >> 3, token_rows(at), :], gu_sem.at[at & 1])

    def h1_copy(at):
        return pltpu.make_async_copy(h1_buf.at[at & 1], h1_hbm.at[token_rows(at - 1), :], h1_sem.at[at & 1])

    @pl.when(step == 0)
    def _():
        signal_entry((core_dev, x_dev, y_dev))
        pltpu.make_async_copy(x_hbm, n_all, in_sem.at[0]).start()
        pltpu.make_async_copy(gain_hbm, gain, in_sem.at[1]).start()

        @pl.loop(0, UNITS)
        def _(unit):
            load(unit)

        wait_entry((core_dev, x_dev, y_dev))

        @pl.loop(0, 5)
        def _(unit):
            send_own(unit)

        pltpu.make_async_copy(x_hbm, n_all, in_sem.at[0]).wait()
        pltpu.make_async_copy(gain_hbm, gain, in_sem.at[1]).wait()

        @pl.loop(0, NT)
        def _(t):
            rows_t = rows_of(t * TM, TM)
            h = n_all[rows_t, :].astype(F32)
            n_all[rows_t, :] = (h * inv_rms_of(h) * gain[0:1, :]).astype(BF16)

        forward_x(0)
        forward_y(0)
        complete(0)

    @pl.when(jnp.logical_and(step & 3 == 1, (step >> 2) + 1 < UNITS))
    def _():
        unit = (step >> 2) + 1

        @pl.when(unit + 4 < UNITS)
        def _():
            send_own(unit + 4)

        forward_x(unit)

    @pl.when(jnp.logical_and(step & 3 == 2, jnp.logical_and(step >= 4, step >> 2 < UNITS)))
    def _():
        forward_y(step >> 2)

    @pl.when(jnp.logical_and(tok == 0, jnp.logical_and(step > 0, step <= last)))
    def _():
        complete(tile)

    @pl.when(jnp.logical_and(step & 3 == 3, step >> 2 >= NF))
    def _():
        complete(step >> 2)

    @pl.when(jnp.logical_and(step >= last + 1 - NT, step <= last))
    def _():
        x_copy(step + 1).start()

    @pl.when(step >= 2)
    def _():
        gu_copy(step - 2).wait()

    rows = rows_of(tok * TM, TM)
    prev_rows = rows_of((prev & 7) * TM, TM)

    gu = dot_nn(n_all[rows, :], wgu[tile]).astype(BF16)
    acc[prev_rows, :] = jnp.where(prev_tile == 0, 0.0, acc[prev_rows, :]) + dot_nn(prods[1 - side], wd[prev_tile])
    gu_buf[side] = gu
    gate = gu[:, :FT].astype(F32)
    prods[side] = (gate * sigmoid(gate) * gu[:, FT:].astype(F32)).astype(BF16)

    @pl.when(step <= last)
    def _():
        gu_copy(step).start()

    @pl.when(step > last + 1 - NT)
    def _():
        x_copy(step).wait()

        @pl.when(step > last + 3 - NT)
        def _():
            h1_copy(step - 2).wait()

        h1_buf[side] = (x_buf[side].astype(F32) + acc[prev_rows, :]).astype(BF16)
        h1_copy(step).start()

    @pl.when(step == last + 1)
    def _():
        gu_copy(last).wait()
        for at in (last, last + 1):
            h1_copy(at).wait()

        for kind in range(5):
            for i, ref in enumerate((wgu, wd)):
                size = (GR, 128)[i] // (1 if kind == 0 else 2)
                sent = ref.at[:, pl.ds(0, size), :]
                pltpu.make_async_copy(sent, sent, send_sem.at[kind, i]).wait()
        pltpu.make_async_copy(wgu, wgu_hbm, out_sem.at[0]).wait()
        pltpu.make_async_copy(wd, wd_hbm, out_sem.at[1]).wait()


def forward_gather(x, gain, wg_sh, wu_sh, wd_sh):
    any_spec = pl.BlockSpec(memory_space=pl.ANY)
    dma = pltpu.SemaphoreType.DMA
    pair = dma((2,))
    return pl.pallas_call(
        gather_kernel,
        grid=(NF * NT + 1,),
        in_specs=[any_spec] * 5,
        out_specs=[any_spec] * 4,
        out_shape=[jax.ShapeDtypeStruct((NF, TOK, 2 * FT), BF16), jax.ShapeDtypeStruct((TOK, D), BF16),
                   jax.ShapeDtypeStruct((UNITS, D, 2 * FT), BF16), jax.ShapeDtypeStruct((UNITS, FT, D), BF16)],
        scratch_shapes=[pltpu.VMEM((TOK, D), BF16), pltpu.VMEM((TOK, D), F32), pltpu.VMEM((2, TM, FT), BF16),
                        pltpu.VMEM((UNITS, D, 2 * FT), BF16), pltpu.VMEM((UNITS, FT, D), BF16),
                        pltpu.VMEM((2, TM, D), BF16), pltpu.VMEM((2, TM, 2 * FT), BF16), pltpu.VMEM((2, TM, D), BF16),
                        pltpu.VMEM((LAYERS, D), F32),
                        dma((UNITS, 2)), dma((5, 2)), dma((UNITS, 5, 2)), dma((2,)),
                        pair, pair, pair, pair],
        compiler_params=pltpu.CompilerParams(collective_id=1, has_side_effects=True, vmem_limit_bytes=VMEM_MAX),
        cost_estimate=pl.CostEstimate(flops=6 * TOK * D * FF, bytes_accessed=100 << 20, transcendentals=0),
        name="forward_gather",
    )(x, gain, wg_sh, wu_sh, wd_sh)


def grads_kernel(h1_hbm, x_hbm, gain_hbm, wgu_hbm, wd_hbm, gu_hbm, dy_hbm, y_hbm, prod_hbm, parts, fin, gain_sum_hbm,
                 n_all, cot_all, dn_all, acc_gu, acc_d, prod_buf, wgu, wd, h_buf, gu_buf, gain, gain_out,
                 gain_acc, own, r_core, sum_c, r_x, sum_x, r_y, sum_y, r_z, done, g_recv, g_zrecv,
                 in_sem, dy_sem, wgu_sem, wd_sem, h_sem, gu_sem, y_sem, prod_sem, ring_sem, part_sem,
                 own_sem, core_send, core_recv, x_send, x_recv, y_send, y_recv,
                 z_send, z_recv, dz_send, dz_recv, dy_send, dy_recv, fin_sem, gs_send, gs_recv, gz_send, gz_recv):
    step = pl.program_id(0)
    wide = step >> 3
    tok = step & 7
    side = step & 1
    slot = wide & 1
    in_l1 = wide < NF
    in_main = wide < TILES
    in_l0 = jnp.logical_and(wide >= NF, in_main)
    first_tile = wide == TILES
    last_tile = wide == TILES + NF - 1
    reads_h = (wide == 0) | (wide == NF - 1) | (wide == NF) | (wide == TILES)
    shard, xx, cc, yy, zz = place()
    core_dev = {"fsdp": 2 * xx + (1 - cc)}
    x_dev = {"fsdp": 2 * (1 - xx) + cc}
    y_dev = {"replica": 1 - yy}
    z_devs = [{"dp": (zz + k) % 4} for k in (1, 2, 3)]

    def remote(src, dst, send, recv, dev):
        return pltpu.make_async_remote_copy(src_ref=src, dst_ref=dst, send_sem=send, recv_sem=recv, device_id=dev,
                                            device_id_type=MESH_ID)

    half_mine = rows_of(yy * 192, 192)
    half_other = rows_of((1 - yy) * 192, 192)

    def core_copy(j):
        return remote(parts.at[j, 1 - cc], r_core.at[j & 1], core_send, core_recv.at[j & 1], core_dev)

    def own_copy(j):
        return pltpu.make_async_copy(parts.at[j, cc], own, own_sem)

    def x_copy(j):
        return remote(sum_c.at[j & 1, 1 - xx], r_x.at[j & 3], x_send.at[j & 1], x_recv.at[j & 3], x_dev)

    def y_copy(j):
        return remote(sum_x.at[j & 1, half_other, :], r_y.at[j & 3], y_send.at[j & 1], y_recv.at[j & 3], y_dev)

    def z_copies(j):
        return [remote(sum_y.at[j & 1, rows_of(((zz + k + 1) % 4) * 48, 48), :], r_z.at[j & 3, k],
                       z_send.at[j & 1, k], z_recv.at[j & 3, k], dev) for k, dev in enumerate(z_devs)]

    def quarter(q):
        return rows_of(yy * 192 + q * 48, 48)

    def done_z_copies(j):
        ref = done.at[j & 7, quarter(zz), :]
        return [remote(ref, ref, dz_send.at[j & 1, k], dz_recv.at[j & 3, k], dev) for k, dev in enumerate(z_devs)]

    def done_y_copy(j):
        ref = done.at[j & 7, half_mine, :]
        return remote(ref, ref, dy_send.at[j & 1], dy_recv.at[j & 3], y_dev)

    def fin_copy(j):
        return pltpu.make_async_copy(done.at[j & 7], fin.at[j], fin_sem.at[j & 1])

    def stage0(j):
        whole = parts.at[j]
        pltpu.make_async_copy(whole, whole, part_sem.at[lax.rem(j, 3)]).wait()
        own_copy(j).start()
        core_copy(j).start()

    def stage1(j):
        own_copy(j).wait()
        core_copy(j).wait()
        sum_c[j & 1] = own[...] + r_core[j & 1]
        x_copy(j).start()

    def stage2(j):
        x_copy(j).wait()
        sum_x[j & 1] = sum_c[j & 1, xx] + r_x[j & 3]
        y_copy(j).start()

    def stage3(j):
        y_copy(j).wait()
        sum_y[j & 1] = sum_x[j & 1, half_mine, :] + r_y[j & 3]
        for copy in z_copies(j):
            copy.start()

    def stage4(j):
        for copy in z_copies(j):
            copy.wait()
        done[j & 7, quarter(zz), :] = ((sum_y[j & 1, rows_of(zz * 48, 48), :] + r_z[j & 3, 0])
                                       + (r_z[j & 3, 1] + r_z[j & 3, 2]))
        for copy in done_z_copies(j):
            copy.start()

    def stage5(j):
        for copy in done_z_copies(j):
            copy.wait()
        done_y_copy(j).start()

    def stage6(j):
        done_y_copy(j).wait()
        fin_copy(j).start()

    def stage7(j):
        fin_copy(j).wait()

    even_stages = ((O7, stage7), (O3, stage3), (O2, stage2), (0, stage0))
    odd_stages = ((O6, stage6), (O5, stage5), (O4, stage4), (O1, stage1))

    def run_beat(count, parity):
        for offset, stage in (even_stages, odd_stages)[parity]:
            job = (count - offset) >> 1

            @pl.when(jnp.logical_and(count >= offset, job < JOBS))
            def _():
                stage(job)

    def write_parts(which, at):
        for s in range(4):
            for k in range(3):
                pltpu.make_async_copy(acc_d.at[at, pl.ds(s * 128, 128), pl.ds(k * 256, 256)],
                                      parts.at[3 * which, s % 2, s // 2, pl.ds(k * 128, 128), :],
                                      part_sem.at[0]).start()
            for m in range(2):
                for k in range(2):
                    pltpu.make_async_copy(acc_gu.at[at, pl.ds(s * GR, GR), pl.ds(m * FT + k * 256, 256)],
                                          parts.at[3 * which + 1 + m, s % 2, s // 2, pl.ds(k * 192, 192), :],
                                          part_sem.at[1 + m]).start()

    def unit_of(at):
        return jnp.where(at < NF, at + NF, at - NF)

    def wgu_copy(at):
        return pltpu.make_async_copy(wgu_hbm.at[unit_of(at)], wgu.at[at & 1], wgu_sem.at[at & 1])

    def wd_copy(at):
        return pltpu.make_async_copy(wd_hbm.at[unit_of(at)], wd.at[at & 1], wd_sem.at[at & 1])

    def token_rows(at):
        return rows_of((at & 7) * TM, TM)

    def h_copy(at, source):
        return pltpu.make_async_copy(source.at[token_rows(at), :], h_buf.at[at & 1], h_sem.at[at & 1])

    def gu_copy(at):
        return pltpu.make_async_copy(gu_hbm.at[(at >> 3) - NF, token_rows(at), :], gu_buf.at[at & 1], gu_sem.at[at & 1])

    def y_copy_out(at):
        return pltpu.make_async_copy(n_all.at[token_rows(at), :], y_hbm.at[token_rows(at), :], y_sem.at[0])

    def prefetch(at):
        tile = at >> 3
        reads_h1 = jnp.logical_or(tile == 0, tile == NF - 1)

        @pl.when(reads_h1)
        def _():
            h_copy(at, h1_hbm).start()

        @pl.when(jnp.logical_or(tile == NF, tile == TILES))
        def _():
            h_copy(at, x_hbm).start()

        @pl.when(jnp.logical_and(tile >= NF, tile < TILES))
        def _():
            gu_copy(at).start()

    def dy_copy(at):
        return pltpu.make_async_copy(dy_hbm.at[token_rows(at), :], cot_all.at[token_rows(at), :], dy_sem.at[at & 7])

    partners = (core_dev, x_dev, y_dev, *z_devs)

    @pl.when(step == 0)
    def _():
        signal_entry(partners)
        wgu_copy(0).start()
        wd_copy(0).start()
        prefetch(step)
        pltpu.make_async_copy(gain_hbm, gain, in_sem.at[1]).start()
        for at in range(NT):
            dy_copy(at).start()
        gain_acc[0] = jnp.zeros_like(gain_acc[0])
        pltpu.make_async_copy(gain_hbm, gain, in_sem.at[1]).wait()

    @pl.when(step == NT)
    def _():
        wait_entry(partners)

    @pl.when(wide == 0)
    def _():
        dy_copy(step).wait()

    @pl.when(tok == 0)
    def _():
        wd_copy(wide).wait()

        @pl.when(in_main)
        def _():
            wgu_copy(wide).wait()

        @pl.when(wide + 1 < TILES + NF)
        def _():
            wd_copy(wide + 1).start()

        @pl.when(wide + 1 < TILES)
        def _():
            wgu_copy(wide + 1).start()

        @pl.when(jnp.logical_and(wide >= 1, wide <= TILES))
        def _():
            write_parts(wide - 1, (wide - 1) & 1)

    @pl.when(step + 1 < STEPS)
    def _():
        prefetch(step + 1)

    @pl.when(reads_h)
    def _():
        h_copy(step, h1_hbm).wait()

    @pl.when(in_l0)
    def _():
        gu_copy(step).wait()

    beat = 6 * (wide - 1) + tok - jnp.where(tok > 4, 2, 1)
    reducing = jnp.logical_and(jnp.logical_and(in_main, wide >= 1), tok & 3 != 0)
    for parity in range(2):
        @pl.when(jnp.logical_and(reducing, beat & 1 == parity))
        def _():
            run_beat(beat, parity)

    rows = rows_of(tok * TM, TM)
    first_tok = tok == 0

    def prod_copy(at):
        return pltpu.make_async_copy(prod_buf.at[at & 1], prod_hbm.at[at >> 3, token_rows(at), :], prod_sem.at[at & 1])

    def ring(at):
        return cot_all.at[token_rows(at), pl.ds(0, FT)]

    def prod_load(at):
        return pltpu.make_async_copy(prod_hbm.at[at >> 3, token_rows(at), :], ring(at), ring_sem.at[at & 7])

    @pl.when(jnp.logical_and(step >= 2, step < NF * NT + 2))
    def _():
        prod_copy(step - 2).wait()

    def add_gain(row, dn, h, inv):
        part = jnp.sum(dn * h * inv, axis=0, keepdims=True)
        gain_acc[0, row:row + 1, :] = jnp.where(first_tok, 0.0, gain_acc[0, row:row + 1, :]) + part

    def backward(layer, first, last):
        cot = cot_all[rows, :]
        gain_row = gain[layer:layer + 1, :]
        if first or last:
            h = h_buf[side].astype(F32)
            inv = inv_rms_of(h)
        if first:
            normed = (h * inv * gain_row).astype(BF16)
            n_all[rows, :] = normed
        else:
            normed = n_all[rows, :]
        gu = dot_nn(normed, wgu[slot]).astype(BF16) if layer else gu_buf[side]
        d_prod = dot_nt(cot, wd[slot]).astype(BF16).astype(F32)
        gate = gu[:, :FT].astype(F32)
        up = gu[:, FT:].astype(F32)
        sig = sigmoid(gate)
        silu = gate * sig
        prod = (silu * up).astype(BF16)
        if layer:
            prod_buf[side] = prod
        d_up = (d_prod * silu).astype(BF16)
        d_gate = ((d_prod * up) * (sig + silu * (1.0 - sig))).astype(BF16)
        d_gu = jnp.concatenate([d_gate, d_up], axis=1)

        def add_weights():
            acc_d[slot] = jnp.where(first_tok, 0.0, acc_d[slot]) + dot_tn(prod, cot)
            acc_gu[slot] = jnp.where(first_tok, 0.0, acc_gu[slot]) + dot_tn(normed, d_gu)

        if not last:
            add_weights()
        dn = dot_nt(d_gu, wgu[slot])
        if not first:
            dn = dn_all[rows, :] + dn
        if last:
            dn = dn.astype(BF16).astype(F32)
            add_gain(layer, dn, h, inv)
            scaled = dn * gain_row
            back = inv * scaled - h * (inv * inv * inv * jnp.mean(scaled * h, axis=-1, keepdims=True))
            cot_all[rows, :] = (cot.astype(F32) + back).astype(BF16)
            add_weights()
        else:
            dn_all[rows, :] = dn

    @pl.when(wide == 0)
    def _():
        backward(1, True, False)

    @pl.when(jnp.logical_and(wide > 0, wide < NF - 1))
    def _():
        backward(1, False, False)

    @pl.when(wide == NF - 1)
    def _():
        backward(1, False, True)

    @pl.when(in_l1)
    def _():
        prod_copy(step).start()

    @pl.when(wide == NF)
    def _():
        backward(0, True, False)

    @pl.when(jnp.logical_and(wide > NF, in_main))
    def _():
        backward(0, False, False)

    @pl.when(wide == TILES)
    def _():
        h = h_buf[side].astype(F32)
        add_gain(0, dn_all[rows, :].astype(BF16).astype(F32), h, inv_rms_of(h))

    def gain_copy(leg, dev):
        return remote(gain_acc.at[leg], g_recv.at[leg], gs_send.at[leg], gs_recv.at[leg], dev)

    def gain_z_copies():
        return [remote(g_zrecv.at[zz], g_zrecv.at[zz], gz_send.at[k], gz_recv.at[k], dev)
                for k, dev in enumerate(z_devs)]

    legs = (core_dev, x_dev, y_dev)
    rest = step - MAIN

    h1_load = pltpu.make_async_copy(h1_hbm, n_all, y_sem.at[1])

    @pl.when(rest == 0)
    def _():
        for at in range(AHEAD):
            prod_load(at).start()
        h1_load.start()

    @pl.when(rest >= 0)
    def _():
        full = rest < SLOW
        late = 6 * (TILES - 1) + jnp.where(full, lax.div(rest, 3), rest - SLOW + SLOW // 3)
        due = jnp.logical_or(jnp.logical_not(full), lax.rem(rest, 3) == 0)

        @pl.when(rest + AHEAD < NF * NT)
        def _():
            prod_load(rest + AHEAD).start()

        for parity in range(2):
            @pl.when(jnp.logical_and(due, jnp.logical_and(late & 1 == parity, late < BEATS)))
            def _():
                run_beat(late, parity)

        for leg, at in enumerate((9, 13, 27, 35)):
            @pl.when(rest == at)
            def _():
                if leg > 0:
                    gain_copy(leg - 1, legs[leg - 1]).wait()
                    total = gain_acc[leg - 1] + g_recv[leg - 1]
                    if leg < 3:
                        gain_acc[leg] = total
                    else:
                        g_zrecv[zz] = total
                if leg < 3:
                    gain_copy(leg, legs[leg]).start()
                else:
                    for copy in gain_z_copies():
                        copy.start()

        @pl.when(rest == 45)
        def _():
            for copy in gain_z_copies():
                copy.wait()
            gain_out[...] = ((g_zrecv[0] + g_zrecv[1]) + (g_zrecv[2] + g_zrecv[3]))[:LAYERS]
            pltpu.make_async_copy(gain_out, gain_sum_hbm, in_sem.at[1]).start()

        prod_load(rest).wait()
        dn_all[rows, :] = jnp.where(first_tile, 0.0, dn_all[rows, :]) + dot_nn(ring(rest)[...], wd[slot])

        @pl.when(last_tile)
        def _():
            @pl.when(first_tok)
            def _():
                h1_load.wait()

            n_all[rows, :] = (n_all[rows, :].astype(F32) + dn_all[rows, :]).astype(BF16)
            y_copy_out(step).start()

        @pl.when(step == STEPS - 1)
        def _():
            pltpu.make_async_copy(gain_out, gain_sum_hbm, in_sem.at[1]).wait()
            pltpu.make_async_copy(n_all, y_hbm, y_sem.at[0]).wait()


def backward_reduce(h1, x, gain, wgu, wd, gu0, dy):
    any_spec = pl.BlockSpec(memory_space=pl.ANY)
    dma = pltpu.SemaphoreType.DMA
    pair, trio, quad, ring = (dma((n,)) for n in (2, 3, 4, 8))
    two_blk = pltpu.VMEM((2, *BLK), F32)
    z_sems = (dma((2, 3)), dma((4, 3)))
    return pl.pallas_call(
        grads_kernel,
        grid=(STEPS,),
        in_specs=[any_spec] * 7,
        out_specs=[any_spec] * 5,
        out_shape=[jax.ShapeDtypeStruct((TOK, D), BF16), jax.ShapeDtypeStruct((NF, TOK, FT), BF16),
                   jax.ShapeDtypeStruct((JOBS, 2, 2, *BLK), F32), jax.ShapeDtypeStruct((JOBS, *BLK), F32),
                   jax.ShapeDtypeStruct((LAYERS, D), F32)],
        scratch_shapes=[pltpu.VMEM((TOK, D), BF16), pltpu.VMEM((TOK, D), BF16), pltpu.VMEM((TOK, D), F32),
                        pltpu.VMEM((2, D, 2 * FT), F32), pltpu.VMEM((2, FT, D), F32), pltpu.VMEM((2, TM, FT), BF16),
                        pltpu.VMEM((2, D, 2 * FT), BF16), pltpu.VMEM((2, FT, D), BF16), pltpu.VMEM((2, TM, D), BF16),
                        pltpu.VMEM((2, TM, 2 * FT), BF16), pltpu.VMEM((LAYERS, D), F32),
                        pltpu.VMEM((LAYERS, D), F32), pltpu.VMEM((3, 8, D), F32),
                        two_blk, pltpu.VMEM((2, 2, *BLK), F32), pltpu.VMEM((2, 2, *BLK), F32),
                        pltpu.VMEM((4, *BLK), F32), two_blk, pltpu.VMEM((4, 192, 256), F32),
                        pltpu.VMEM((2, 192, 256), F32), pltpu.VMEM((4, 3, 48, 256), F32), pltpu.VMEM((8, *BLK), F32),
                        pltpu.VMEM((3, 8, D), F32), pltpu.VMEM((4, 8, D), F32),
                        pair, ring, pair, pair, pair, pair, pair, pair, ring, trio,
                        dma, dma, pair, pair, quad, pair, quad, *z_sems, *z_sems, pair, quad, pair, trio, trio, trio, trio],
        compiler_params=pltpu.CompilerParams(collective_id=2, has_side_effects=True, vmem_limit_bytes=VMEM_MAX),
        cost_estimate=pl.CostEstimate(flops=30 * TOK * D * FF, bytes_accessed=320 << 20, transcendentals=0),
        name="backward_reduce",
    )(h1, x, gain, wgu, wd, gu0, dy)


def place_kernel(fin, y_in, gain_in, d_gate, d_up, d_down, y_out, gain_out, stage, y_stage, load_sem, store_sem, y_load, y_store):
    def fin_load(job):
        return pltpu.make_async_copy(fin.at[job], stage.at[job], load_sem.at[job])

    def fin_store(job):
        layer = 1 - job // (3 * NF)
        col = (job // 3 % NF) * 128
        src = stage.at[job]
        sem = store_sem.at[job]
        if job % 3 == 0:
            for k in range(3):
                pltpu.make_async_copy(src.at[pl.ds(k * 128, 128), :],
                                      d_down.at[layer, pl.ds(col, 128), pl.ds(k * 256, 256)], sem).start()
        else:
            dst = d_gate if job % 3 == 1 else d_up
            for k in range(2):
                for g in range(2):
                    pltpu.make_async_copy(src.at[pl.ds(k * GR, GR), pl.ds(g * 128, 128)],
                                          dst.at[layer, :, pl.ds((2 * k + g) * D + col, 128)], sem).start()

    def y_copies(t):
        rows = pl.ds(t * TM, TM)
        return (pltpu.make_async_copy(y_in.at[rows, :], y_stage.at[rows, :], y_load.at[t]),
                pltpu.make_async_copy(y_stage.at[rows, :], y_out.at[rows, :], y_store.at[t]))

    gain_out[...] = gain_in[...]
    for t in range(NT):
        y_copies(t)[0].start()
    for job in range(JOBS):
        fin_load(job).start()
    for t in range(NT):
        load, store = y_copies(t)
        load.wait()
        store.start()
    for job in range(JOBS):
        fin_load(job).wait()
        fin_store(job)
    for t in range(NT):
        y_copies(t)[1].wait()
    for job in range(JOBS):
        src = stage.at[job]
        pltpu.make_async_copy(src, src, store_sem.at[job]).wait()


def place_grads(fin, y, gain_sum):
    any_spec = pl.BlockSpec(memory_space=pl.ANY)
    shard = jax.ShapeDtypeStruct((LAYERS, GR, FF), F32)
    dma = pltpu.SemaphoreType.DMA
    return pl.pallas_call(
        place_kernel,
        in_specs=[any_spec, any_spec, pl.BlockSpec(memory_space=pltpu.VMEM)],
        out_specs=[*[any_spec] * 4, pl.BlockSpec(memory_space=pltpu.VMEM)],
        out_shape=[shard, shard, jax.ShapeDtypeStruct((LAYERS, D, D), F32), jax.ShapeDtypeStruct((TOK, D), BF16),
                   jax.ShapeDtypeStruct((LAYERS, D), F32)],
        scratch_shapes=[pltpu.VMEM((JOBS, *BLK), F32), pltpu.VMEM((TOK, D), BF16), dma((JOBS,)), dma((JOBS,)),
                        dma((NT,)), dma((NT,))],
        compiler_params=pltpu.CompilerParams(vmem_limit_bytes=VMEM_MAX),
        cost_estimate=pl.CostEstimate(flops=0, bytes_accessed=41 << 20, transcendentals=0),
        name="place_grads",
    )(fin, y, gain_sum)


def solution(mesh):
    tok_spec = P(TOKEN_AXES, None)
    shard_spec = P(None, "fsdp", None)
    full_spec = P(None, None)

    def device_step(x_local, dy_local, w_gate_sh, w_up_sh, w_down_sh, norm_gain):
        gu0, h1, wgu, wd = forward_gather(x_local, norm_gain, w_gate_sh, w_up_sh, w_down_sh)
        y_local, _, _, fin, gain_sum = backward_reduce(h1, x_local, norm_gain, wgu, wd, gu0, dy_local)
        d_gate, d_up, d_down, y_out, d_gain = place_grads(fin, y_local, gain_sum)
        return y_out, d_gate, d_up, d_down, d_gain

    return jax.shard_map(device_step, mesh=mesh,
                         in_specs=(tok_spec, tok_spec, shard_spec, shard_spec, shard_spec, full_spec),
                         out_specs=(tok_spec, shard_spec, shard_spec, shard_spec, full_spec), check_vma=False)
```

```python
import jax
import jax.numpy as jnp
from jax import lax
from jax.experimental import pallas as pl
from jax.experimental.pallas import tpu as pltpu
from jax.sharding import PartitionSpec as P

NORM_EPS = 1e-6
TOKEN_AXES = ("dp", "replica", "fsdp")
MESH_ID = pl.DeviceIdType.MESH
BF16 = jnp.bfloat16
F32 = jnp.float32

TOK = 4096
D = 768
FF = 3072
LAYERS = 2
TM = 512
NT = TOK // TM
FT = 512
NF = FF // FT
GR = D // 4
UNITS = LAYERS * NF
TILES = LAYERS * NF
JOBS = 3 * TILES
BLK = (384, 256)
VMEM_MAX = 67043328
O1, O2, O3, O4, O5, O6, O7 = 1, 4, 6, 9, 13, 17, 18
BEATS = 2 * (JOBS - 1) + O7 + 1
MAIN = LAYERS * NF * NT
STEPS = MAIN + NF * NT + 8
AHEAD = 6
PACE = 3
SLOW = 42


def dot_nn(a, b):
    return lax.dot_general(a, b, (((1,), (0,)), ((), ())), preferred_element_type=F32)


def dot_nt(a, b):
    return lax.dot_general(a, b, (((1,), (1,)), ((), ())), preferred_element_type=F32)


def dot_tn(a, b):
    return lax.dot_general(a, b, (((0,), (0,)), ((), ())), preferred_element_type=F32)


def sigmoid(v):
    return 0.5 * jnp.tanh(0.5 * v) + 0.5


def inv_rms_of(h):
    return lax.rsqrt(jnp.mean(h * h, axis=-1, keepdims=True) + NORM_EPS)


def rows_of(start, size):
    return pl.ds(pl.multiple_of(start, size), size)


def place():
    shard = lax.axis_index("fsdp")
    return shard, shard // 2, shard % 2, lax.axis_index("replica"), lax.axis_index("dp")


def signal_entry(partners):
    for partner in partners:
        pl.semaphore_signal(pltpu.get_barrier_semaphore(), inc=1, device_id=partner, device_id_type=MESH_ID)


def wait_entry(partners):
    pl.semaphore_wait(pltpu.get_barrier_semaphore(), len(partners))


def gather_kernel(x_hbm, gain_hbm, wg_sh, wu_sh, wd_sh, gu_hbm, h1_hbm, wgu_hbm, wd_hbm,
                  n_all, acc, prods, wgu, wd, x_buf, gu_buf, h1_buf, gain, load_sem, send_sem, recv_sem, out_sem,
                  x_sem, gu_sem, h1_sem, in_sem):
    step = pl.program_id(0)
    last = NF * NT - 1
    tile = jnp.minimum(step, last) >> 3
    tok = step & 7
    prev = jnp.maximum(step - 1, 0)
    prev_tile = prev >> 3
    side = step & 1
    shard, xx, cc, yy, zz = place()
    core_dev = {"fsdp": 2 * xx + (1 - cc)}
    x_dev = {"fsdp": 2 * (1 - xx) + cc}
    y_dev = {"replica": 1 - yy}
    core_sh = 2 * xx + (1 - cc)
    x_sh = 2 * (1 - xx) + cc
    far_sh = 2 * (1 - xx) + (1 - cc)
    both = (0, 1)

    def part(unit, owner, half):
        if half is None:
            return wgu.at[unit, rows_of(owner * GR, GR), :], wd.at[unit, rows_of(owner * 128, 128), :]
        return (wgu.at[unit, rows_of(owner * GR + half * 96, 96), :],
                wd.at[unit, rows_of(owner * 128 + half * 64, 64), :])

    def message(unit, kind, owner, half, dev, which=both):
        refs = part(unit, owner, half)
        return [pltpu.make_async_remote_copy(src_ref=refs[i], dst_ref=refs[i], send_sem=send_sem.at[kind, i],
                                             recv_sem=recv_sem.at[unit, kind, i], device_id=dev,
                                             device_id_type=MESH_ID)
                for i in which]

    def send(*args):
        for copy in message(*args):
            copy.start()

    def arrived(*args):
        for copy in message(*args):
            copy.wait_recv()

    def load(unit):
        layer = lax.div(unit, NF)
        col = lax.rem(unit, NF) * 128
        for group in range(4):
            cols = rows_of(group * D + col, 128)
            pltpu.make_async_copy(wg_sh.at[layer, :, cols],
                                  wgu.at[unit, rows_of(shard * GR, GR), pl.ds(group * 128, 128)],
                                  load_sem.at[unit, 0]).start()
            pltpu.make_async_copy(wu_sh.at[layer, :, cols],
                                  wgu.at[unit, rows_of(shard * GR, GR), pl.ds(FT + group * 128, 128)],
                                  load_sem.at[unit, 0]).start()
        pltpu.make_async_copy(wd_sh.at[layer, rows_of(col, 128), :],
                              wd.at[unit, rows_of(shard * 128, 128), :], load_sem.at[unit, 1]).start()

    def send_own(unit):
        own = part(unit, shard, None)
        for i in both:
            pltpu.make_async_copy(own[i], own[i], load_sem.at[unit, i]).wait()
            send(unit, 1, shard, yy, x_dev, (i,))
            send(unit, 0, shard, None, core_dev, (i,))

    def forward_x(unit, which=both):
        for i in which:
            arrived(unit, 1, x_sh, yy, x_dev, (i,))
            send(unit, 2, x_sh, yy, y_dev, (i,))
            send(unit, 3, x_sh, yy, core_dev, (i,))

    def forward_y(unit, which=both):
        for i in which:
            arrived(unit, 2, x_sh, 1 - yy, y_dev, (i,))
            send(unit, 4, x_sh, 1 - yy, core_dev, (i,))

    def out_copy(unit, i):
        if i == 0:
            return pltpu.make_async_copy(wgu.at[unit], wgu_hbm.at[unit], out_sem.at[0])
        return pltpu.make_async_copy(wd.at[unit], wd_hbm.at[unit], out_sem.at[1])

    def complete(unit, which=both):
        for i in which:
            arrived(unit, 0, core_sh, None, core_dev, (i,))
            arrived(unit, 3, far_sh, yy, core_dev, (i,))
            arrived(unit, 4, far_sh, 1 - yy, core_dev, (i,))
            out_copy(unit, i).start()

    def token_rows(at):
        return rows_of((at & 7) * TM, TM)

    def x_copy(at):
        return pltpu.make_async_copy(x_hbm.at[token_rows(at - 1), :], x_buf.at[at & 1], x_sem.at[at & 1])

    def gu_copy(at):
        return pltpu.make_async_copy(gu_buf.at[at & 1], gu_hbm.at[at >> 3, token_rows(at), :], gu_sem.at[at & 1])

    def h1_copy(at):
        return pltpu.make_async_copy(h1_buf.at[at & 1], h1_hbm.at[token_rows(at - 1), :], h1_sem.at[at & 1])

    @pl.when(step == 0)
    def _():
        signal_entry((core_dev, x_dev, y_dev))
        pltpu.make_async_copy(x_hbm, n_all, in_sem.at[0]).start()
        pltpu.make_async_copy(gain_hbm, gain, in_sem.at[1]).start()

        @pl.loop(0, UNITS)
        def _(unit):
            load(unit)

        wait_entry((core_dev, x_dev, y_dev))

        @pl.loop(0, 5)
        def _(unit):
            send_own(unit)

        pltpu.make_async_copy(x_hbm, n_all, in_sem.at[0]).wait()
        pltpu.make_async_copy(gain_hbm, gain, in_sem.at[1]).wait()

        @pl.loop(0, NT)
        def _(t):
            rows_t = rows_of(t * TM, TM)
            h = n_all[rows_t, :].astype(F32)
            n_all[rows_t, :] = (h * inv_rms_of(h) * gain[0:1, :]).astype(BF16)

        forward_x(0)
        forward_y(0)
        complete(0)

    @pl.when(jnp.logical_and(step & 3 == 1, (step >> 2) + 1 < UNITS))
    def _():
        unit = (step >> 2) + 1

        @pl.when(unit + 4 < UNITS)
        def _():
            send_own(unit + 4)

        forward_x(unit)

    @pl.when(jnp.logical_and(step & 3 == 2, jnp.logical_and(step >= 4, step >> 2 < UNITS)))
    def _():
        forward_y(step >> 2)

    @pl.when(jnp.logical_and(tok == 0, jnp.logical_and(step > 0, step <= last)))
    def _():
        complete(tile)

    @pl.when(jnp.logical_and(step & 3 == 3, step >> 2 >= NF))
    def _():
        complete(step >> 2)

    @pl.when(jnp.logical_and(step >= last + 1 - NT, step <= last))
    def _():
        x_copy(step + 1).start()

    @pl.when(step >= 2)
    def _():
        gu_copy(step - 2).wait()

    rows = rows_of(tok * TM, TM)
    prev_rows = rows_of((prev & 7) * TM, TM)

    gu = dot_nn(n_all[rows, :], wgu[tile]).astype(BF16)
    acc[prev_rows, :] = jnp.where(prev_tile == 0, 0.0, acc[prev_rows, :]) + dot_nn(prods[1 - side], wd[prev_tile])
    gu_buf[side] = gu
    gate = gu[:, :FT].astype(F32)
    prods[side] = (gate * sigmoid(gate) * gu[:, FT:].astype(F32)).astype(BF16)

    @pl.when(step <= last)
    def _():
        gu_copy(step).start()

    @pl.when(step > last + 1 - NT)
    def _():
        x_copy(step).wait()

        @pl.when(step > last + 3 - NT)
        def _():
            h1_copy(step - 2).wait()

        h1_buf[side] = (x_buf[side].astype(F32) + acc[prev_rows, :]).astype(BF16)
        h1_copy(step).start()

    @pl.when(step == last + 1)
    def _():
        gu_copy(last).wait()
        for at in (last, last + 1):
            h1_copy(at).wait()

        for kind in range(5):
            for i, ref in enumerate((wgu, wd)):
                size = (GR, 128)[i] // (1 if kind == 0 else 2)
                sent = ref.at[:, pl.ds(0, size), :]
                pltpu.make_async_copy(sent, sent, send_sem.at[kind, i]).wait()
        pltpu.make_async_copy(wgu, wgu_hbm, out_sem.at[0]).wait()
        pltpu.make_async_copy(wd, wd_hbm, out_sem.at[1]).wait()


def forward_gather(x, gain, wg_sh, wu_sh, wd_sh):
    any_spec = pl.BlockSpec(memory_space=pl.ANY)
    dma = pltpu.SemaphoreType.DMA
    pair = dma((2,))
    return pl.pallas_call(
        gather_kernel,
        grid=(NF * NT + 1,),
        in_specs=[any_spec] * 5,
        out_specs=[any_spec] * 4,
        out_shape=[jax.ShapeDtypeStruct((NF, TOK, 2 * FT), BF16), jax.ShapeDtypeStruct((TOK, D), BF16),
                   jax.ShapeDtypeStruct((UNITS, D, 2 * FT), BF16), jax.ShapeDtypeStruct((UNITS, FT, D), BF16)],
        scratch_shapes=[pltpu.VMEM((TOK, D), BF16), pltpu.VMEM((TOK, D), F32), pltpu.VMEM((2, TM, FT), BF16),
                        pltpu.VMEM((UNITS, D, 2 * FT), BF16), pltpu.VMEM((UNITS, FT, D), BF16),
                        pltpu.VMEM((2, TM, D), BF16), pltpu.VMEM((2, TM, 2 * FT), BF16), pltpu.VMEM((2, TM, D), BF16),
                        pltpu.VMEM((LAYERS, D), F32),
                        dma((UNITS, 2)), dma((5, 2)), dma((UNITS, 5, 2)), dma((2,)),
                        pair, pair, pair, pair],
        compiler_params=pltpu.CompilerParams(collective_id=1, has_side_effects=True, vmem_limit_bytes=VMEM_MAX),
        cost_estimate=pl.CostEstimate(flops=6 * TOK * D * FF, bytes_accessed=100 << 20, transcendentals=0),
        name="forward_gather",
    )(x, gain, wg_sh, wu_sh, wd_sh)


def grads_kernel(h1_hbm, x_hbm, gain_hbm, wgu_hbm, wd_hbm, gu_hbm, dy_hbm, y_hbm, prod_hbm, parts, fin, gain_sum_hbm,
                 n_all, cot_all, dn_all, acc_gu, acc_d, prod_buf, wgu, wd, h_buf, gu_buf, gain, gain_out,
                 gain_acc, own, r_core, sum_c, r_x, sum_x, r_y, sum_y, r_z, done, g_recv, g_zrecv,
                 in_sem, dy_sem, wgu_sem, wd_sem, h_sem, gu_sem, y_sem, prod_sem, ring_sem, part_sem,
                 own_sem, core_send, core_recv, x_send, x_recv, y_send, y_recv,
                 z_send, z_recv, dz_send, dz_recv, dy_send, dy_recv, fin_sem, gs_send, gs_recv, gz_send, gz_recv):
    step = pl.program_id(0)
    wide = step >> 3
    tok = step & 7
    side = step & 1
    slot = wide & 1
    in_l1 = wide < NF
    in_main = wide < TILES
    in_l0 = jnp.logical_and(wide >= NF, in_main)
    first_tile = wide == TILES
    last_tile = wide == TILES + NF - 1
    reads_h = (wide == 0) | (wide == NF - 1) | (wide == NF) | (wide == TILES)
    shard, xx, cc, yy, zz = place()
    core_dev = {"fsdp": 2 * xx + (1 - cc)}
    x_dev = {"fsdp": 2 * (1 - xx) + cc}
    y_dev = {"replica": 1 - yy}
    z_devs = [{"dp": (zz + k) % 4} for k in (1, 2, 3)]

    def remote(src, dst, send, recv, dev):
        return pltpu.make_async_remote_copy(src_ref=src, dst_ref=dst, send_sem=send, recv_sem=recv, device_id=dev,
                                            device_id_type=MESH_ID)

    half_mine = rows_of(yy * 192, 192)
    half_other = rows_of((1 - yy) * 192, 192)

    def core_copy(j):
        return remote(parts.at[j, 1 - cc], r_core.at[j & 1], core_send, core_recv.at[j & 1], core_dev)

    def own_copy(j):
        return pltpu.make_async_copy(parts.at[j, cc], own, own_sem)

    def x_copy(j):
        return remote(sum_c.at[j & 1, 1 - xx], r_x.at[j & 3], x_send.at[j & 1], x_recv.at[j & 3], x_dev)

    def y_copy(j):
        return remote(sum_x.at[j & 1, half_other, :], r_y.at[j & 3], y_send.at[j & 1], y_recv.at[j & 3], y_dev)

    def z_copies(j):
        return [remote(sum_y.at[j & 1, rows_of(((zz + k + 1) % 4) * 48, 48), :], r_z.at[j & 3, k],
                       z_send.at[j & 1, k], z_recv.at[j & 3, k], dev) for k, dev in enumerate(z_devs)]

    def quarter(q):
        return rows_of(yy * 192 + q * 48, 48)

    def done_z_copies(j):
        ref = done.at[j & 7, quarter(zz), :]
        return [remote(ref, ref, dz_send.at[j & 1, k], dz_recv.at[j & 3, k], dev) for k, dev in enumerate(z_devs)]

    def done_y_copy(j):
        ref = done.at[j & 7, half_mine, :]
        return remote(ref, ref, dy_send.at[j & 1], dy_recv.at[j & 3], y_dev)

    def fin_copy(j):
        return pltpu.make_async_copy(done.at[j & 7], fin.at[j], fin_sem.at[j & 1])

    def stage0(j):
        whole = parts.at[j]
        pltpu.make_async_copy(whole, whole, part_sem.at[lax.rem(j, 3)]).wait()
        own_copy(j).start()
        core_copy(j).start()

    def stage1(j):
        own_copy(j).wait()
        core_copy(j).wait()
        sum_c[j & 1] = own[...] + r_core[j & 1]
        x_copy(j).start()

    def stage2(j):
        x_copy(j).wait()
        sum_x[j & 1] = sum_c[j & 1, xx] + r_x[j & 3]
        y_copy(j).start()

    def stage3(j):
        y_copy(j).wait()
        sum_y[j & 1] = sum_x[j & 1, half_mine, :] + r_y[j & 3]
        for copy in z_copies(j):
            copy.start()

    def stage4(j):
        for copy in z_copies(j):
            copy.wait()
        done[j & 7, quarter(zz), :] = ((sum_y[j & 1, rows_of(zz * 48, 48), :] + r_z[j & 3, 0])
                                       + (r_z[j & 3, 1] + r_z[j & 3, 2]))
        for copy in done_z_copies(j):
            copy.start()

    def stage5(j):
        for copy in done_z_copies(j):
            copy.wait()
        done_y_copy(j).start()

    def stage6(j):
        done_y_copy(j).wait()
        fin_copy(j).start()

    def stage7(j):
        fin_copy(j).wait()

    even_stages = ((O7, stage7), (O3, stage3), (O2, stage2), (0, stage0))
    odd_stages = ((O6, stage6), (O5, stage5), (O4, stage4), (O1, stage1))

    def run_beat(count, parity):
        for offset, stage in (even_stages, odd_stages)[parity]:
            job = (count - offset) >> 1

            @pl.when(jnp.logical_and(count >= offset, job < JOBS))
            def _():
                stage(job)

    def write_parts(which, at):
        for s in range(4):
            for k in range(3):
                pltpu.make_async_copy(acc_d.at[at, pl.ds(s * 128, 128), pl.ds(k * 256, 256)],
                                      parts.at[3 * which, s % 2, s // 2, pl.ds(k * 128, 128), :],
                                      part_sem.at[0]).start()
            for m in range(2):
                for k in range(2):
                    pltpu.make_async_copy(acc_gu.at[at, pl.ds(s * GR, GR), pl.ds(m * FT + k * 256, 256)],
                                          parts.at[3 * which + 1 + m, s % 2, s // 2, pl.ds(k * 192, 192), :],
                                          part_sem.at[1 + m]).start()

    def unit_of(at):
        return jnp.where(at < NF, at + NF, at - NF)

    def wgu_copy(at):
        return pltpu.make_async_copy(wgu_hbm.at[unit_of(at)], wgu.at[at & 1], wgu_sem.at[at & 1])

    def wd_copy(at):
        return pltpu.make_async_copy(wd_hbm.at[unit_of(at)], wd.at[at & 1], wd_sem.at[at & 1])

    def token_rows(at):
        return rows_of((at & 7) * TM, TM)

    def h_copy(at, source):
        return pltpu.make_async_copy(source.at[token_rows(at), :], h_buf.at[at & 1], h_sem.at[at & 1])

    def gu_copy(at):
        return pltpu.make_async_copy(gu_hbm.at[(at >> 3) - NF, token_rows(at), :], gu_buf.at[at & 1], gu_sem.at[at & 1])

    def y_copy_out(at):
        return pltpu.make_async_copy(n_all.at[token_rows(at), :], y_hbm.at[token_rows(at), :], y_sem.at[0])

    def prefetch(at):
        tile = at >> 3
        reads_h1 = jnp.logical_or(tile == 0, tile == NF - 1)

        @pl.when(reads_h1)
        def _():
            h_copy(at, h1_hbm).start()

        @pl.when(jnp.logical_or(tile == NF, tile == TILES))
        def _():
            h_copy(at, x_hbm).start()

        @pl.when(jnp.logical_and(tile >= NF, tile < TILES))
        def _():
            gu_copy(at).start()

    def dy_copy(at):
        return pltpu.make_async_copy(dy_hbm.at[token_rows(at), :], cot_all.at[token_rows(at), :], dy_sem.at[at & 7])

    partners = (core_dev, x_dev, y_dev, *z_devs)

    @pl.when(step == 0)
    def _():
        signal_entry(partners)
        wgu_copy(0).start()
        wd_copy(0).start()
        prefetch(step)
        pltpu.make_async_copy(gain_hbm, gain, in_sem.at[1]).start()
        for at in range(NT):
            dy_copy(at).start()
        gain_acc[0] = jnp.zeros_like(gain_acc[0])
        pltpu.make_async_copy(gain_hbm, gain, in_sem.at[1]).wait()

    @pl.when(step == NT)
    def _():
        wait_entry(partners)

    @pl.when(wide == 0)
    def _():
        dy_copy(step).wait()

    @pl.when(jnp.logical_and(tok == 0, wide < TILES + NF))
    def _():
        wd_copy(wide).wait()

        @pl.when(in_main)
        def _():
            wgu_copy(wide).wait()

        @pl.when(wide + 1 < TILES + NF)
        def _():
            wd_copy(wide + 1).start()

        @pl.when(wide + 1 < TILES)
        def _():
            wgu_copy(wide + 1).start()

        @pl.when(jnp.logical_and(wide >= 1, wide <= TILES))
        def _():
            write_parts(wide - 1, (wide - 1) & 1)

    @pl.when(step + 1 < STEPS)
    def _():
        prefetch(step + 1)

    @pl.when(reads_h)
    def _():
        h_copy(step, h1_hbm).wait()

    @pl.when(in_l0)
    def _():
        gu_copy(step).wait()

    beat = 6 * (wide - 1) + tok - jnp.where(tok > 4, 2, 1)
    reducing = jnp.logical_and(jnp.logical_and(in_main, wide >= 1), tok & 3 != 0)
    for parity in range(2):
        @pl.when(jnp.logical_and(reducing, beat & 1 == parity))
        def _():
            run_beat(beat, parity)

    rows = rows_of(tok * TM, TM)
    first_tok = tok == 0

    def prod_copy(at):
        return pltpu.make_async_copy(prod_buf.at[at & 1], prod_hbm.at[at >> 3, token_rows(at), :], prod_sem.at[at & 1])

    def ring(at):
        return cot_all.at[token_rows(at), pl.ds(0, FT)]

    def prod_load(at):
        return pltpu.make_async_copy(prod_hbm.at[at >> 3, token_rows(at), :], ring(at), ring_sem.at[at & 7])

    @pl.when(jnp.logical_and(step >= 2, step < NF * NT + 2))
    def _():
        prod_copy(step - 2).wait()

    def add_gain(row, dn, h, inv):
        part = jnp.sum(dn * h * inv, axis=0, keepdims=True)
        gain_acc[0, row:row + 1, :] = jnp.where(first_tok, 0.0, gain_acc[0, row:row + 1, :]) + part

    def backward(layer, first, last):
        cot = cot_all[rows, :]
        gain_row = gain[layer:layer + 1, :]
        if first or last:
            h = h_buf[side].astype(F32)
            inv = inv_rms_of(h)
        if first:
            normed = (h * inv * gain_row).astype(BF16)
            n_all[rows, :] = normed
        else:
            normed = n_all[rows, :]
        gu = dot_nn(normed, wgu[slot]).astype(BF16) if layer else gu_buf[side]
        d_prod = dot_nt(cot, wd[slot]).astype(BF16).astype(F32)
        gate = gu[:, :FT].astype(F32)
        up = gu[:, FT:].astype(F32)
        sig = sigmoid(gate)
        silu = gate * sig
        prod = (silu * up).astype(BF16)
        if layer:
            prod_buf[side] = prod
        d_up = (d_prod * silu).astype(BF16)
        d_gate = ((d_prod * up) * (sig + silu * (1.0 - sig))).astype(BF16)
        d_gu = jnp.concatenate([d_gate, d_up], axis=1)

        def add_weights():
            acc_d[slot] = jnp.where(first_tok, 0.0, acc_d[slot]) + dot_tn(prod, cot)
            acc_gu[slot] = jnp.where(first_tok, 0.0, acc_gu[slot]) + dot_tn(normed, d_gu)

        if not last:
            add_weights()
        dn = dot_nt(d_gu, wgu[slot])
        if not first:
            dn = dn_all[rows, :] + dn
        if last:
            dn = dn.astype(BF16).astype(F32)
            add_gain(layer, dn, h, inv)
            scaled = dn * gain_row
            back = inv * scaled - h * (inv * inv * inv * jnp.mean(scaled * h, axis=-1, keepdims=True))
            cot_all[rows, :] = (cot.astype(F32) + back).astype(BF16)
            add_weights()
        else:
            dn_all[rows, :] = dn

    @pl.when(wide == 0)
    def _():
        backward(1, True, False)

    @pl.when(jnp.logical_and(wide > 0, wide < NF - 1))
    def _():
        backward(1, False, False)

    @pl.when(wide == NF - 1)
    def _():
        backward(1, False, True)

    @pl.when(in_l1)
    def _():
        prod_copy(step).start()

    @pl.when(wide == NF)
    def _():
        backward(0, True, False)

    @pl.when(jnp.logical_and(wide > NF, in_main))
    def _():
        backward(0, False, False)

    @pl.when(wide == TILES)
    def _():
        h = h_buf[side].astype(F32)
        add_gain(0, dn_all[rows, :].astype(BF16).astype(F32), h, inv_rms_of(h))

    def gain_copy(leg, dev):
        return remote(gain_acc.at[leg], g_recv.at[leg], gs_send.at[leg], gs_recv.at[leg], dev)

    def gain_z_copies():
        return [remote(g_zrecv.at[zz], g_zrecv.at[zz], gz_send.at[k], gz_recv.at[k], dev)
                for k, dev in enumerate(z_devs)]

    legs = (core_dev, x_dev, y_dev)
    rest = step - MAIN

    h1_load = pltpu.make_async_copy(h1_hbm, n_all, y_sem.at[1])

    @pl.when(rest == 0)
    def _():
        for at in range(AHEAD):
            prod_load(at).start()
        h1_load.start()

    @pl.when(rest >= 0)
    def _():
        full = rest < SLOW
        late = 6 * (TILES - 1) + jnp.where(full, lax.div(rest, PACE), rest - SLOW + SLOW // PACE)
        due = jnp.logical_or(jnp.logical_not(full), lax.rem(rest, PACE) == 0)

        @pl.when(rest + AHEAD < NF * NT)
        def _():
            prod_load(rest + AHEAD).start()

        for parity in range(2):
            @pl.when(jnp.logical_and(due, jnp.logical_and(late & 1 == parity, late < BEATS)))
            def _():
                run_beat(late, parity)

        for leg, at in enumerate((9, 13, 27, 35)):
            @pl.when(rest == at)
            def _():
                if leg > 0:
                    gain_copy(leg - 1, legs[leg - 1]).wait()
                    total = gain_acc[leg - 1] + g_recv[leg - 1]
                    if leg < 3:
                        gain_acc[leg] = total
                    else:
                        g_zrecv[zz] = total
                if leg < 3:
                    gain_copy(leg, legs[leg]).start()
                else:
                    for copy in gain_z_copies():
                        copy.start()

        @pl.when(rest == 45)
        def _():
            for copy in gain_z_copies():
                copy.wait()
            gain_out[...] = ((g_zrecv[0] + g_zrecv[1]) + (g_zrecv[2] + g_zrecv[3]))[:LAYERS]
            pltpu.make_async_copy(gain_out, gain_sum_hbm, in_sem.at[1]).start()

        @pl.when(rest < NF * NT)
        def _():
            prod_load(rest).wait()
            dn_all[rows, :] = jnp.where(first_tile, 0.0, dn_all[rows, :]) + dot_nn(ring(rest)[...], wd[slot])

            @pl.when(last_tile)
            def _():
                @pl.when(first_tok)
                def _():
                    h1_load.wait()

                n_all[rows, :] = (n_all[rows, :].astype(F32) + dn_all[rows, :]).astype(BF16)
                y_copy_out(step).start()

        @pl.when(step == STEPS - 1)
        def _():
            pltpu.make_async_copy(gain_out, gain_sum_hbm, in_sem.at[1]).wait()
            pltpu.make_async_copy(n_all, y_hbm, y_sem.at[0]).wait()


def backward_reduce(h1, x, gain, wgu, wd, gu0, dy):
    any_spec = pl.BlockSpec(memory_space=pl.ANY)
    dma = pltpu.SemaphoreType.DMA
    pair, trio, quad, ring = (dma((n,)) for n in (2, 3, 4, 8))
    two_blk = pltpu.VMEM((2, *BLK), F32)
    z_sems = (dma((2, 3)), dma((4, 3)))
    return pl.pallas_call(
        grads_kernel,
        grid=(STEPS,),
        in_specs=[any_spec] * 7,
        out_specs=[any_spec] * 5,
        out_shape=[jax.ShapeDtypeStruct((TOK, D), BF16), jax.ShapeDtypeStruct((NF, TOK, FT), BF16),
                   jax.ShapeDtypeStruct((JOBS, 2, 2, *BLK), F32), jax.ShapeDtypeStruct((JOBS, *BLK), F32),
                   jax.ShapeDtypeStruct((LAYERS, D), F32)],
        scratch_shapes=[pltpu.VMEM((TOK, D), BF16), pltpu.VMEM((TOK, D), BF16), pltpu.VMEM((TOK, D), F32),
                        pltpu.VMEM((2, D, 2 * FT), F32), pltpu.VMEM((2, FT, D), F32), pltpu.VMEM((2, TM, FT), BF16),
                        pltpu.VMEM((2, D, 2 * FT), BF16), pltpu.VMEM((2, FT, D), BF16), pltpu.VMEM((2, TM, D), BF16),
                        pltpu.VMEM((2, TM, 2 * FT), BF16), pltpu.VMEM((LAYERS, D), F32),
                        pltpu.VMEM((LAYERS, D), F32), pltpu.VMEM((3, 8, D), F32),
                        two_blk, pltpu.VMEM((2, 2, *BLK), F32), pltpu.VMEM((2, 2, *BLK), F32),
                        pltpu.VMEM((4, *BLK), F32), two_blk, pltpu.VMEM((4, 192, 256), F32),
                        pltpu.VMEM((2, 192, 256), F32), pltpu.VMEM((4, 3, 48, 256), F32), pltpu.VMEM((8, *BLK), F32),
                        pltpu.VMEM((3, 8, D), F32), pltpu.VMEM((4, 8, D), F32),
                        pair, ring, pair, pair, pair, pair, pair, pair, ring, trio,
                        dma, dma, pair, pair, quad, pair, quad, *z_sems, *z_sems, pair, quad, pair, trio, trio, trio, trio],
        compiler_params=pltpu.CompilerParams(collective_id=2, has_side_effects=True, vmem_limit_bytes=VMEM_MAX),
        cost_estimate=pl.CostEstimate(flops=30 * TOK * D * FF, bytes_accessed=320 << 20, transcendentals=0),
        name="backward_reduce",
    )(h1, x, gain, wgu, wd, gu0, dy)


def place_kernel(fin, y_in, gain_in, d_gate, d_up, d_down, y_out, gain_out, stage, y_stage, load_sem, store_sem, y_load, y_store):
    def fin_load(job):
        return pltpu.make_async_copy(fin.at[job], stage.at[job], load_sem.at[job])

    def fin_store(job):
        layer = 1 - job // (3 * NF)
        col = (job // 3 % NF) * 128
        src = stage.at[job]
        sem = store_sem.at[job]
        if job % 3 == 0:
            for k in range(3):
                pltpu.make_async_copy(src.at[pl.ds(k * 128, 128), :],
                                      d_down.at[layer, pl.ds(col, 128), pl.ds(k * 256, 256)], sem).start()
        else:
            dst = d_gate if job % 3 == 1 else d_up
            for k in range(2):
                for g in range(2):
                    pltpu.make_async_copy(src.at[pl.ds(k * GR, GR), pl.ds(g * 128, 128)],
                                          dst.at[layer, :, pl.ds((2 * k + g) * D + col, 128)], sem).start()

    def y_copies(t):
        rows = pl.ds(t * TM, TM)
        return (pltpu.make_async_copy(y_in.at[rows, :], y_stage.at[rows, :], y_load.at[t]),
                pltpu.make_async_copy(y_stage.at[rows, :], y_out.at[rows, :], y_store.at[t]))

    gain_out[...] = gain_in[...]
    for t in range(NT):
        y_copies(t)[0].start()
    for job in range(JOBS):
        fin_load(job).start()
    for t in range(NT):
        load, store = y_copies(t)
        load.wait()
        store.start()
    for job in range(JOBS):
        fin_load(job).wait()
        fin_store(job)
    for t in range(NT):
        y_copies(t)[1].wait()
    for job in range(JOBS):
        src = stage.at[job]
        pltpu.make_async_copy(src, src, store_sem.at[job]).wait()


def place_grads(fin, y, gain_sum):
    any_spec = pl.BlockSpec(memory_space=pl.ANY)
    shard = jax.ShapeDtypeStruct((LAYERS, GR, FF), F32)
    dma = pltpu.SemaphoreType.DMA
    return pl.pallas_call(
        place_kernel,
        in_specs=[any_spec, any_spec, pl.BlockSpec(memory_space=pltpu.VMEM)],
        out_specs=[*[any_spec] * 4, pl.BlockSpec(memory_space=pltpu.VMEM)],
        out_shape=[shard, shard, jax.ShapeDtypeStruct((LAYERS, D, D), F32), jax.ShapeDtypeStruct((TOK, D), BF16),
                   jax.ShapeDtypeStruct((LAYERS, D), F32)],
        scratch_shapes=[pltpu.VMEM((JOBS, *BLK), F32), pltpu.VMEM((TOK, D), BF16), dma((JOBS,)), dma((JOBS,)),
                        dma((NT,)), dma((NT,))],
        compiler_params=pltpu.CompilerParams(vmem_limit_bytes=VMEM_MAX),
        cost_estimate=pl.CostEstimate(flops=0, bytes_accessed=41 << 20, transcendentals=0),
        name="place_grads",
    )(fin, y, gain_sum)


def solution(mesh):
    tok_spec = P(TOKEN_AXES, None)
    shard_spec = P(None, "fsdp", None)
    full_spec = P(None, None)

    def device_step(x_local, dy_local, w_gate_sh, w_up_sh, w_down_sh, norm_gain):
        gu0, h1, wgu, wd = forward_gather(x_local, norm_gain, w_gate_sh, w_up_sh, w_down_sh)
        y_local, _, _, fin, gain_sum = backward_reduce(h1, x_local, norm_gain, wgu, wd, gu0, dy_local)
        d_gate, d_up, d_down, y_out, d_gain = place_grads(fin, y_local, gain_sum)
        return y_out, d_gate, d_up, d_down, d_gain

    return jax.shard_map(device_step, mesh=mesh,
                         in_specs=(tok_spec, tok_spec, shard_spec, shard_spec, shard_spec, full_spec),
                         out_specs=(tok_spec, shard_spec, shard_spec, shard_spec, full_spec), check_vma=False)
```

```python
import jax
import jax.numpy as jnp
from jax import lax
from jax.experimental import pallas as pl
from jax.experimental.pallas import tpu as pltpu
from jax.sharding import PartitionSpec as P

NORM_EPS = 1e-6
TOKEN_AXES = ("dp", "replica", "fsdp")
MESH_ID = pl.DeviceIdType.MESH
BF16 = jnp.bfloat16
F32 = jnp.float32

TOK = 4096
D = 768
FF = 3072
LAYERS = 2
TM = 512
NT = TOK // TM
FT = 512
NF = FF // FT
GR = D // 4
UNITS = LAYERS * NF
TILES = LAYERS * NF
JOBS = 3 * TILES
BLK = (384, 256)
VMEM_MAX = 67043328
O1, O2, O3, O4, O5, O6, O7 = 1, 4, 6, 9, 13, 17, 18
BEATS = 2 * (JOBS - 1) + O7 + 1
MAIN = LAYERS * NF * NT
STEPS = MAIN + NF * NT + 8
AHEAD = 6
Z_ORDER = (0, 2, 1)
PACE = 3
SLOW = 42


def dot_nn(a, b):
    return lax.dot_general(a, b, (((1,), (0,)), ((), ())), preferred_element_type=F32)


def dot_nt(a, b):
    return lax.dot_general(a, b, (((1,), (1,)), ((), ())), preferred_element_type=F32)


def dot_tn(a, b):
    return lax.dot_general(a, b, (((0,), (0,)), ((), ())), preferred_element_type=F32)


def sigmoid(v):
    return 0.5 * jnp.tanh(0.5 * v) + 0.5


def inv_rms_of(h):
    return lax.rsqrt(jnp.mean(h * h, axis=-1, keepdims=True) + NORM_EPS)


def rows_of(start, size):
    return pl.ds(pl.multiple_of(start, size), size)


def place():
    shard = lax.axis_index("fsdp")
    return shard, shard // 2, shard % 2, lax.axis_index("replica"), lax.axis_index("dp")


def signal_entry(partners):
    for partner in partners:
        pl.semaphore_signal(pltpu.get_barrier_semaphore(), inc=1, device_id=partner, device_id_type=MESH_ID)


def wait_entry(partners):
    pl.semaphore_wait(pltpu.get_barrier_semaphore(), len(partners))


def gather_kernel(x_hbm, gain_hbm, wg_sh, wu_sh, wd_sh, gu_hbm, h1_hbm, wgu_hbm, wd_hbm,
                  n_all, acc, prods, wgu, wd, x_buf, gu_buf, h1_buf, gain, load_sem, send_sem, recv_sem, out_sem,
                  x_sem, gu_sem, h1_sem, in_sem):
    step = pl.program_id(0)
    last = NF * NT - 1
    tile = jnp.minimum(step, last) >> 3
    tok = step & 7
    prev = jnp.maximum(step - 1, 0)
    prev_tile = prev >> 3
    side = step & 1
    shard, xx, cc, yy, zz = place()
    core_dev = {"fsdp": 2 * xx + (1 - cc)}
    x_dev = {"fsdp": 2 * (1 - xx) + cc}
    y_dev = {"replica": 1 - yy}
    core_sh = 2 * xx + (1 - cc)
    x_sh = 2 * (1 - xx) + cc
    far_sh = 2 * (1 - xx) + (1 - cc)
    both = (0, 1)

    def part(unit, owner, half):
        if half is None:
            return wgu.at[unit, rows_of(owner * GR, GR), :], wd.at[unit, rows_of(owner * 128, 128), :]
        return (wgu.at[unit, rows_of(owner * GR + half * 96, 96), :],
                wd.at[unit, rows_of(owner * 128 + half * 64, 64), :])

    def message(unit, kind, owner, half, dev, which=both):
        refs = part(unit, owner, half)
        return [pltpu.make_async_remote_copy(src_ref=refs[i], dst_ref=refs[i], send_sem=send_sem.at[kind, i],
                                             recv_sem=recv_sem.at[unit, kind, i], device_id=dev,
                                             device_id_type=MESH_ID)
                for i in which]

    def send(*args):
        for copy in message(*args):
            copy.start()

    def arrived(*args):
        for copy in message(*args):
            copy.wait_recv()

    def load(unit):
        layer = lax.div(unit, NF)
        col = lax.rem(unit, NF) * 128
        for group in range(4):
            cols = rows_of(group * D + col, 128)
            pltpu.make_async_copy(wg_sh.at[layer, :, cols],
                                  wgu.at[unit, rows_of(shard * GR, GR), pl.ds(group * 128, 128)],
                                  load_sem.at[unit, 0]).start()
            pltpu.make_async_copy(wu_sh.at[layer, :, cols],
                                  wgu.at[unit, rows_of(shard * GR, GR), pl.ds(FT + group * 128, 128)],
                                  load_sem.at[unit, 0]).start()
        pltpu.make_async_copy(wd_sh.at[layer, rows_of(col, 128), :],
                              wd.at[unit, rows_of(shard * 128, 128), :], load_sem.at[unit, 1]).start()

    def send_own(unit):
        own = part(unit, shard, None)
        for i in both:
            pltpu.make_async_copy(own[i], own[i], load_sem.at[unit, i]).wait()
            send(unit, 1, shard, yy, x_dev, (i,))
            send(unit, 0, shard, None, core_dev, (i,))

    def forward_x(unit, which=both):
        for i in which:
            arrived(unit, 1, x_sh, yy, x_dev, (i,))
            send(unit, 2, x_sh, yy, y_dev, (i,))
            send(unit, 3, x_sh, yy, core_dev, (i,))

    def forward_y(unit, which=both):
        for i in which:
            arrived(unit, 2, x_sh, 1 - yy, y_dev, (i,))
            send(unit, 4, x_sh, 1 - yy, core_dev, (i,))

    def out_copy(unit, i):
        if i == 0:
            return pltpu.make_async_copy(wgu.at[unit], wgu_hbm.at[unit], out_sem.at[0])
        return pltpu.make_async_copy(wd.at[unit], wd_hbm.at[unit], out_sem.at[1])

    def complete(unit, which=both):
        for i in which:
            arrived(unit, 0, core_sh, None, core_dev, (i,))
            arrived(unit, 3, far_sh, yy, core_dev, (i,))
            arrived(unit, 4, far_sh, 1 - yy, core_dev, (i,))
            out_copy(unit, i).start()

    def token_rows(at):
        return rows_of((at & 7) * TM, TM)

    def x_copy(at):
        return pltpu.make_async_copy(x_hbm.at[token_rows(at - 1), :], x_buf.at[at & 1], x_sem.at[at & 1])

    def gu_copy(at):
        return pltpu.make_async_copy(gu_buf.at[at & 1], gu_hbm.at[at >> 3, token_rows(at), :], gu_sem.at[at & 1])

    def h1_copy(at):
        return pltpu.make_async_copy(h1_buf.at[at & 1], h1_hbm.at[token_rows(at - 1), :], h1_sem.at[at & 1])

    @pl.when(step == 0)
    def _():
        signal_entry((core_dev, x_dev, y_dev))
        pltpu.make_async_copy(x_hbm, n_all, in_sem.at[0]).start()
        pltpu.make_async_copy(gain_hbm, gain, in_sem.at[1]).start()

        @pl.loop(0, UNITS)
        def _(unit):
            load(unit)

        wait_entry((core_dev, x_dev, y_dev))

        @pl.loop(0, 5)
        def _(unit):
            send_own(unit)

        pltpu.make_async_copy(x_hbm, n_all, in_sem.at[0]).wait()
        pltpu.make_async_copy(gain_hbm, gain, in_sem.at[1]).wait()

        @pl.loop(0, NT)
        def _(t):
            rows_t = rows_of(t * TM, TM)
            h = n_all[rows_t, :].astype(F32)
            n_all[rows_t, :] = (h * inv_rms_of(h) * gain[0:1, :]).astype(BF16)

        forward_x(0)
        forward_y(0)
        complete(0)

    @pl.when(jnp.logical_and(step & 3 == 1, (step >> 2) + 1 < UNITS))
    def _():
        unit = (step >> 2) + 1

        @pl.when(unit + 4 < UNITS)
        def _():
            send_own(unit + 4)

        forward_x(unit)

    @pl.when(jnp.logical_and(step & 3 == 2, jnp.logical_and(step >= 4, step >> 2 < UNITS)))
    def _():
        forward_y(step >> 2)

    @pl.when(jnp.logical_and(tok == 0, jnp.logical_and(step > 0, step <= last)))
    def _():
        complete(tile)

    @pl.when(jnp.logical_and(step & 3 == 3, step >> 2 >= NF))
    def _():
        complete(step >> 2)

    @pl.when(jnp.logical_and(step >= last + 1 - NT, step <= last))
    def _():
        x_copy(step + 1).start()

    @pl.when(step >= 2)
    def _():
        gu_copy(step - 2).wait()

    rows = rows_of(tok * TM, TM)
    prev_rows = rows_of((prev & 7) * TM, TM)

    gu = dot_nn(n_all[rows, :], wgu[tile]).astype(BF16)
    acc[prev_rows, :] = jnp.where(prev_tile == 0, 0.0, acc[prev_rows, :]) + dot_nn(prods[1 - side], wd[prev_tile])
    gu_buf[side] = gu
    gate = gu[:, :FT].astype(F32)
    prods[side] = (gate * sigmoid(gate) * gu[:, FT:].astype(F32)).astype(BF16)

    @pl.when(step <= last)
    def _():
        gu_copy(step).start()

    @pl.when(step > last + 1 - NT)
    def _():
        x_copy(step).wait()

        @pl.when(step > last + 3 - NT)
        def _():
            h1_copy(step - 2).wait()

        h1_buf[side] = (x_buf[side].astype(F32) + acc[prev_rows, :]).astype(BF16)
        h1_copy(step).start()

    @pl.when(step == last + 1)
    def _():
        gu_copy(last).wait()
        for at in (last, last + 1):
            h1_copy(at).wait()

        for kind in range(5):
            for i, ref in enumerate((wgu, wd)):
                size = (GR, 128)[i] // (1 if kind == 0 else 2)
                sent = ref.at[:, pl.ds(0, size), :]
                pltpu.make_async_copy(sent, sent, send_sem.at[kind, i]).wait()
        pltpu.make_async_copy(wgu, wgu_hbm, out_sem.at[0]).wait()
        pltpu.make_async_copy(wd, wd_hbm, out_sem.at[1]).wait()


def forward_gather(x, gain, wg_sh, wu_sh, wd_sh):
    any_spec = pl.BlockSpec(memory_space=pl.ANY)
    dma = pltpu.SemaphoreType.DMA
    pair = dma((2,))
    return pl.pallas_call(
        gather_kernel,
        grid=(NF * NT + 1,),
        in_specs=[any_spec] * 5,
        out_specs=[any_spec] * 4,
        out_shape=[jax.ShapeDtypeStruct((NF, TOK, 2 * FT), BF16), jax.ShapeDtypeStruct((TOK, D), BF16),
                   jax.ShapeDtypeStruct((UNITS, D, 2 * FT), BF16), jax.ShapeDtypeStruct((UNITS, FT, D), BF16)],
        scratch_shapes=[pltpu.VMEM((TOK, D), BF16), pltpu.VMEM((TOK, D), F32), pltpu.VMEM((2, TM, FT), BF16),
                        pltpu.VMEM((UNITS, D, 2 * FT), BF16), pltpu.VMEM((UNITS, FT, D), BF16),
                        pltpu.VMEM((2, TM, D), BF16), pltpu.VMEM((2, TM, 2 * FT), BF16), pltpu.VMEM((2, TM, D), BF16),
                        pltpu.VMEM((LAYERS, D), F32),
                        dma((UNITS, 2)), dma((5, 2)), dma((UNITS, 5, 2)), dma((2,)),
                        pair, pair, pair, pair],
        compiler_params=pltpu.CompilerParams(collective_id=1, has_side_effects=True, vmem_limit_bytes=VMEM_MAX),
        cost_estimate=pl.CostEstimate(flops=6 * TOK * D * FF, bytes_accessed=100 << 20, transcendentals=0),
        name="forward_gather",
    )(x, gain, wg_sh, wu_sh, wd_sh)


def grads_kernel(h1_hbm, x_hbm, gain_hbm, wgu_hbm, wd_hbm, gu_hbm, dy_hbm, y_hbm, prod_hbm, parts, fin, gain_sum_hbm,
                 n_all, cot_all, dn_all, acc_gu, acc_d, prod_buf, wgu, wd, h_buf, gu_buf, gain, gain_out,
                 gain_acc, own, r_core, sum_c, r_x, sum_x, r_y, sum_y, r_z, done, g_recv, g_zrecv,
                 in_sem, dy_sem, wgu_sem, wd_sem, h_sem, gu_sem, y_sem, prod_sem, ring_sem, part_sem,
                 own_sem, core_send, core_recv, x_send, x_recv, y_send, y_recv,
                 z_send, z_recv, dz_send, dz_recv, dy_send, dy_recv, fin_sem, gs_send, gs_recv, gz_send, gz_recv):
    step = pl.program_id(0)
    wide = step >> 3
    tok = step & 7
    side = step & 1
    slot = wide & 1
    in_l1 = wide < NF
    in_main = wide < TILES
    in_l0 = jnp.logical_and(wide >= NF, in_main)
    first_tile = wide == TILES
    last_tile = wide == TILES + NF - 1
    reads_h = (wide == 0) | (wide == NF - 1) | (wide == NF) | (wide == TILES)
    shard, xx, cc, yy, zz = place()
    core_dev = {"fsdp": 2 * xx + (1 - cc)}
    x_dev = {"fsdp": 2 * (1 - xx) + cc}
    y_dev = {"replica": 1 - yy}
    z_devs = [{"dp": (zz + k) % 4} for k in (1, 2, 3)]

    def remote(src, dst, send, recv, dev):
        return pltpu.make_async_remote_copy(src_ref=src, dst_ref=dst, send_sem=send, recv_sem=recv, device_id=dev,
                                            device_id_type=MESH_ID)

    half_mine = rows_of(yy * 192, 192)
    half_other = rows_of((1 - yy) * 192, 192)

    def core_copy(j):
        return remote(parts.at[j, 1 - cc], r_core.at[j & 1], core_send, core_recv.at[j & 1], core_dev)

    def own_copy(j):
        return pltpu.make_async_copy(parts.at[j, cc], own, own_sem)

    def x_copy(j):
        return remote(sum_c.at[j & 1, 1 - xx], r_x.at[j & 3], x_send.at[j & 1], x_recv.at[j & 3], x_dev)

    def y_copy(j):
        return remote(sum_x.at[j & 1, half_other, :], r_y.at[j & 3], y_send.at[j & 1], y_recv.at[j & 3], y_dev)

    def z_copies(j):
        return [remote(sum_y.at[j & 1, rows_of(((zz + k + 1) % 4) * 48, 48), :], r_z.at[j & 3, k],
                       z_send.at[j & 1, k], z_recv.at[j & 3, k], dev) for k, dev in enumerate(z_devs)]

    def quarter(q):
        return rows_of(yy * 192 + q * 48, 48)

    def done_z_copies(j):
        ref = done.at[j & 7, quarter(zz), :]
        return [remote(ref, ref, dz_send.at[j & 1, k], dz_recv.at[j & 3, k], dev) for k, dev in enumerate(z_devs)]

    def done_y_copy(j):
        ref = done.at[j & 7, half_mine, :]
        return remote(ref, ref, dy_send.at[j & 1], dy_recv.at[j & 3], y_dev)

    def fin_copy(j):
        return pltpu.make_async_copy(done.at[j & 7], fin.at[j], fin_sem.at[j & 1])

    def stage0(j):
        whole = parts.at[j]
        pltpu.make_async_copy(whole, whole, part_sem.at[lax.rem(j, 3)]).wait()
        own_copy(j).start()
        core_copy(j).start()

    def stage1(j):
        own_copy(j).wait()
        core_copy(j).wait()
        sum_c[j & 1] = own[...] + r_core[j & 1]
        x_copy(j).start()

    def stage2(j):
        x_copy(j).wait()
        sum_x[j & 1] = sum_c[j & 1, xx] + r_x[j & 3]
        y_copy(j).start()

    def stage3(j):
        y_copy(j).wait()
        sum_y[j & 1] = sum_x[j & 1, half_mine, :] + r_y[j & 3]
        copies = z_copies(j)
        for k in Z_ORDER:
            copies[k].start()

    def stage4(j):
        for copy in z_copies(j):
            copy.wait()
        done[j & 7, quarter(zz), :] = ((sum_y[j & 1, rows_of(zz * 48, 48), :] + r_z[j & 3, 0])
                                       + (r_z[j & 3, 1] + r_z[j & 3, 2]))
        copies = done_z_copies(j)
        for k in Z_ORDER:
            copies[k].start()

    def stage5(j):
        for copy in done_z_copies(j):
            copy.wait()
        done_y_copy(j).start()

    def stage6(j):
        done_y_copy(j).wait()
        fin_copy(j).start()

    def stage7(j):
        fin_copy(j).wait()

    even_stages = ((O7, stage7), (O3, stage3), (O2, stage2), (0, stage0))
    odd_stages = ((O6, stage6), (O5, stage5), (O4, stage4), (O1, stage1))

    def run_beat(count, parity):
        for offset, stage in (even_stages, odd_stages)[parity]:
            job = (count - offset) >> 1

            @pl.when(jnp.logical_and(count >= offset, job < JOBS))
            def _():
                stage(job)

    def write_parts(which, at):
        for s in range(4):
            for k in range(3):
                pltpu.make_async_copy(acc_d.at[at, pl.ds(s * 128, 128), pl.ds(k * 256, 256)],
                                      parts.at[3 * which, s % 2, s // 2, pl.ds(k * 128, 128), :],
                                      part_sem.at[0]).start()
            for m in range(2):
                for k in range(2):
                    pltpu.make_async_copy(acc_gu.at[at, pl.ds(s * GR, GR), pl.ds(m * FT + k * 256, 256)],
                                          parts.at[3 * which + 1 + m, s % 2, s // 2, pl.ds(k * 192, 192), :],
                                          part_sem.at[1 + m]).start()

    def unit_of(at):
        return jnp.where(at < NF, at + NF, at - NF)

    def wgu_copy(at):
        return pltpu.make_async_copy(wgu_hbm.at[unit_of(at)], wgu.at[at & 1], wgu_sem.at[at & 1])

    def wd_copy(at):
        return pltpu.make_async_copy(wd_hbm.at[unit_of(at)], wd.at[at & 1], wd_sem.at[at & 1])

    def token_rows(at):
        return rows_of((at & 7) * TM, TM)

    def h_copy(at, source):
        return pltpu.make_async_copy(source.at[token_rows(at), :], h_buf.at[at & 1], h_sem.at[at & 1])

    def gu_copy(at):
        return pltpu.make_async_copy(gu_hbm.at[(at >> 3) - NF, token_rows(at), :], gu_buf.at[at & 1], gu_sem.at[at & 1])

    def y_copy_out(at):
        return pltpu.make_async_copy(n_all.at[token_rows(at), :], y_hbm.at[token_rows(at), :], y_sem.at[0])

    def prefetch(at):
        tile = at >> 3
        reads_h1 = jnp.logical_or(tile == 0, tile == NF - 1)

        @pl.when(reads_h1)
        def _():
            h_copy(at, h1_hbm).start()

        @pl.when(jnp.logical_or(tile == NF, tile == TILES))
        def _():
            h_copy(at, x_hbm).start()

        @pl.when(jnp.logical_and(tile >= NF, tile < TILES))
        def _():
            gu_copy(at).start()

    def dy_copy(at):
        return pltpu.make_async_copy(dy_hbm.at[token_rows(at), :], cot_all.at[token_rows(at), :], dy_sem.at[at & 7])

    partners = (core_dev, x_dev, y_dev, *z_devs)

    @pl.when(step == 0)
    def _():
        signal_entry(partners)
        wgu_copy(0).start()
        wd_copy(0).start()
        prefetch(step)
        pltpu.make_async_copy(gain_hbm, gain, in_sem.at[1]).start()
        for at in range(NT):
            dy_copy(at).start()
        gain_acc[0] = jnp.zeros_like(gain_acc[0])
        pltpu.make_async_copy(gain_hbm, gain, in_sem.at[1]).wait()

    @pl.when(step == NT)
    def _():
        wait_entry(partners)

    @pl.when(wide == 0)
    def _():
        dy_copy(step).wait()

    @pl.when(jnp.logical_and(tok == 0, wide < TILES + NF))
    def _():
        wd_copy(wide).wait()

        @pl.when(in_main)
        def _():
            wgu_copy(wide).wait()

        @pl.when(wide + 1 < TILES + NF)
        def _():
            wd_copy(wide + 1).start()

        @pl.when(wide + 1 < TILES)
        def _():
            wgu_copy(wide + 1).start()

        @pl.when(jnp.logical_and(wide >= 1, wide <= TILES))
        def _():
            write_parts(wide - 1, (wide - 1) & 1)

    @pl.when(step + 1 < STEPS)
    def _():
        prefetch(step + 1)

    @pl.when(reads_h)
    def _():
        h_copy(step, h1_hbm).wait()

    @pl.when(in_l0)
    def _():
        gu_copy(step).wait()

    beat = 6 * (wide - 1) + tok - jnp.where(tok > 4, 2, 1)
    reducing = jnp.logical_and(jnp.logical_and(in_main, wide >= 1), tok & 3 != 0)
    for parity in range(2):
        @pl.when(jnp.logical_and(reducing, beat & 1 == parity))
        def _():
            run_beat(beat, parity)

    rows = rows_of(tok * TM, TM)
    first_tok = tok == 0

    def prod_copy(at):
        return pltpu.make_async_copy(prod_buf.at[at & 1], prod_hbm.at[at >> 3, token_rows(at), :], prod_sem.at[at & 1])

    def ring(at):
        return cot_all.at[token_rows(at), pl.ds(0, FT)]

    def prod_load(at):
        return pltpu.make_async_copy(prod_hbm.at[at >> 3, token_rows(at), :], ring(at), ring_sem.at[at & 7])

    @pl.when(jnp.logical_and(step >= 2, step < NF * NT + 2))
    def _():
        prod_copy(step - 2).wait()

    def add_gain(row, dn, h, inv):
        part = jnp.sum(dn * h * inv, axis=0, keepdims=True)
        gain_acc[0, row:row + 1, :] = jnp.where(first_tok, 0.0, gain_acc[0, row:row + 1, :]) + part

    def backward(layer, first, last):
        cot = cot_all[rows, :]
        gain_row = gain[layer:layer + 1, :]
        if first or last:
            h = h_buf[side].astype(F32)
            inv = inv_rms_of(h)
        if first:
            normed = (h * inv * gain_row).astype(BF16)
            n_all[rows, :] = normed
        else:
            normed = n_all[rows, :]
        gu = dot_nn(normed, wgu[slot]).astype(BF16) if layer else gu_buf[side]
        d_prod = dot_nt(cot, wd[slot]).astype(BF16).astype(F32)
        gate = gu[:, :FT].astype(F32)
        up = gu[:, FT:].astype(F32)
        sig = sigmoid(gate)
        silu = gate * sig
        prod = (silu * up).astype(BF16)
        if layer:
            prod_buf[side] = prod
        d_up = (d_prod * silu).astype(BF16)
        d_gate = ((d_prod * up) * (sig + silu * (1.0 - sig))).astype(BF16)
        d_gu = jnp.concatenate([d_gate, d_up], axis=1)

        def add_weights():
            acc_d[slot] = jnp.where(first_tok, 0.0, acc_d[slot]) + dot_tn(prod, cot)
            acc_gu[slot] = jnp.where(first_tok, 0.0, acc_gu[slot]) + dot_tn(normed, d_gu)

        if not last:
            add_weights()
        dn = dot_nt(d_gu, wgu[slot])
        if not first:
            dn = dn_all[rows, :] + dn
        if last:
            dn = dn.astype(BF16).astype(F32)
            add_gain(layer, dn, h, inv)
            scaled = dn * gain_row
            back = inv * scaled - h * (inv * inv * inv * jnp.mean(scaled * h, axis=-1, keepdims=True))
            cot_all[rows, :] = (cot.astype(F32) + back).astype(BF16)
            add_weights()
        else:
            dn_all[rows, :] = dn

    @pl.when(wide == 0)
    def _():
        backward(1, True, False)

    @pl.when(jnp.logical_and(wide > 0, wide < NF - 1))
    def _():
        backward(1, False, False)

    @pl.when(wide == NF - 1)
    def _():
        backward(1, False, True)

    @pl.when(in_l1)
    def _():
        prod_copy(step).start()

    @pl.when(wide == NF)
    def _():
        backward(0, True, False)

    @pl.when(jnp.logical_and(wide > NF, in_main))
    def _():
        backward(0, False, False)

    @pl.when(wide == TILES)
    def _():
        h = h_buf[side].astype(F32)
        add_gain(0, dn_all[rows, :].astype(BF16).astype(F32), h, inv_rms_of(h))

    def gain_copy(leg, dev):
        return remote(gain_acc.at[leg], g_recv.at[leg], gs_send.at[leg], gs_recv.at[leg], dev)

    def gain_z_copies():
        return [remote(g_zrecv.at[zz], g_zrecv.at[zz], gz_send.at[k], gz_recv.at[k], dev)
                for k, dev in enumerate(z_devs)]

    legs = (core_dev, x_dev, y_dev)
    rest = step - MAIN

    h1_load = pltpu.make_async_copy(h1_hbm, n_all, y_sem.at[1])

    @pl.when(rest == 0)
    def _():
        for at in range(AHEAD):
            prod_load(at).start()
        h1_load.start()

    @pl.when(rest >= 0)
    def _():
        full = rest < SLOW
        late = 6 * (TILES - 1) + jnp.where(full, lax.div(rest, PACE), rest - SLOW + SLOW // PACE)
        due = jnp.logical_or(jnp.logical_not(full), lax.rem(rest, PACE) == 0)

        @pl.when(rest + AHEAD < NF * NT)
        def _():
            prod_load(rest + AHEAD).start()

        for parity in range(2):
            @pl.when(jnp.logical_and(due, jnp.logical_and(late & 1 == parity, late < BEATS)))
            def _():
                run_beat(late, parity)

        for leg, at in enumerate((9, 13, 27, 35)):
            @pl.when(rest == at)
            def _():
                if leg > 0:
                    gain_copy(leg - 1, legs[leg - 1]).wait()
                    total = gain_acc[leg - 1] + g_recv[leg - 1]
                    if leg < 3:
                        gain_acc[leg] = total
                    else:
                        g_zrecv[zz] = total
                if leg < 3:
                    gain_copy(leg, legs[leg]).start()
                else:
                    for copy in gain_z_copies():
                        copy.start()

        @pl.when(rest == 45)
        def _():
            for copy in gain_z_copies():
                copy.wait()
            gain_out[...] = ((g_zrecv[0] + g_zrecv[1]) + (g_zrecv[2] + g_zrecv[3]))[:LAYERS]
            pltpu.make_async_copy(gain_out, gain_sum_hbm, in_sem.at[1]).start()

        @pl.when(rest < NF * NT)
        def _():
            prod_load(rest).wait()
            dn_all[rows, :] = jnp.where(first_tile, 0.0, dn_all[rows, :]) + dot_nn(ring(rest)[...], wd[slot])

            @pl.when(last_tile)
            def _():
                @pl.when(first_tok)
                def _():
                    h1_load.wait()

                n_all[rows, :] = (n_all[rows, :].astype(F32) + dn_all[rows, :]).astype(BF16)
                y_copy_out(step).start()

        @pl.when(step == STEPS - 1)
        def _():
            pltpu.make_async_copy(gain_out, gain_sum_hbm, in_sem.at[1]).wait()
            pltpu.make_async_copy(n_all, y_hbm, y_sem.at[0]).wait()


def backward_reduce(h1, x, gain, wgu, wd, gu0, dy):
    any_spec = pl.BlockSpec(memory_space=pl.ANY)
    dma = pltpu.SemaphoreType.DMA
    pair, trio, quad, ring = (dma((n,)) for n in (2, 3, 4, 8))
    two_blk = pltpu.VMEM((2, *BLK), F32)
    z_sems = (dma((2, 3)), dma((4, 3)))
    return pl.pallas_call(
        grads_kernel,
        grid=(STEPS,),
        in_specs=[any_spec] * 7,
        out_specs=[any_spec] * 5,
        out_shape=[jax.ShapeDtypeStruct((TOK, D), BF16), jax.ShapeDtypeStruct((NF, TOK, FT), BF16),
                   jax.ShapeDtypeStruct((JOBS, 2, 2, *BLK), F32), jax.ShapeDtypeStruct((JOBS, *BLK), F32),
                   jax.ShapeDtypeStruct((LAYERS, D), F32)],
        scratch_shapes=[pltpu.VMEM((TOK, D), BF16), pltpu.VMEM((TOK, D), BF16), pltpu.VMEM((TOK, D), F32),
                        pltpu.VMEM((2, D, 2 * FT), F32), pltpu.VMEM((2, FT, D), F32), pltpu.VMEM((2, TM, FT), BF16),
                        pltpu.VMEM((2, D, 2 * FT), BF16), pltpu.VMEM((2, FT, D), BF16), pltpu.VMEM((2, TM, D), BF16),
                        pltpu.VMEM((2, TM, 2 * FT), BF16), pltpu.VMEM((LAYERS, D), F32),
                        pltpu.VMEM((LAYERS, D), F32), pltpu.VMEM((3, 8, D), F32),
                        two_blk, pltpu.VMEM((2, 2, *BLK), F32), pltpu.VMEM((2, 2, *BLK), F32),
                        pltpu.VMEM((4, *BLK), F32), two_blk, pltpu.VMEM((4, 192, 256), F32),
                        pltpu.VMEM((2, 192, 256), F32), pltpu.VMEM((4, 3, 48, 256), F32), pltpu.VMEM((8, *BLK), F32),
                        pltpu.VMEM((3, 8, D), F32), pltpu.VMEM((4, 8, D), F32),
                        pair, ring, pair, pair, pair, pair, pair, pair, ring, trio,
                        dma, dma, pair, pair, quad, pair, quad, *z_sems, *z_sems, pair, quad, pair, trio, trio, trio, trio],
        compiler_params=pltpu.CompilerParams(collective_id=2, has_side_effects=True, vmem_limit_bytes=VMEM_MAX),
        cost_estimate=pl.CostEstimate(flops=30 * TOK * D * FF, bytes_accessed=320 << 20, transcendentals=0),
        name="backward_reduce",
    )(h1, x, gain, wgu, wd, gu0, dy)


def place_kernel(fin, y_in, gain_in, d_gate, d_up, d_down, y_out, gain_out, stage, y_stage, load_sem, store_sem, y_load, y_store):
    def fin_load(job):
        return pltpu.make_async_copy(fin.at[job], stage.at[job], load_sem.at[job])

    def fin_store(job):
        layer = 1 - job // (3 * NF)
        col = (job // 3 % NF) * 128
        src = stage.at[job]
        sem = store_sem.at[job]
        if job % 3 == 0:
            for k in range(3):
                pltpu.make_async_copy(src.at[pl.ds(k * 128, 128), :],
                                      d_down.at[layer, pl.ds(col, 128), pl.ds(k * 256, 256)], sem).start()
        else:
            dst = d_gate if job % 3 == 1 else d_up
            for k in range(2):
                for g in range(2):
                    pltpu.make_async_copy(src.at[pl.ds(k * GR, GR), pl.ds(g * 128, 128)],
                                          dst.at[layer, :, pl.ds((2 * k + g) * D + col, 128)], sem).start()

    def y_copies(t):
        rows = pl.ds(t * TM, TM)
        return (pltpu.make_async_copy(y_in.at[rows, :], y_stage.at[rows, :], y_load.at[t]),
                pltpu.make_async_copy(y_stage.at[rows, :], y_out.at[rows, :], y_store.at[t]))

    gain_out[...] = gain_in[...]
    for t in range(NT):
        y_copies(t)[0].start()
    for job in range(JOBS):
        fin_load(job).start()
    for t in range(NT):
        load, store = y_copies(t)
        load.wait()
        store.start()
    for job in range(JOBS):
        fin_load(job).wait()
        fin_store(job)
    for t in range(NT):
        y_copies(t)[1].wait()
    for job in range(JOBS):
        src = stage.at[job]
        pltpu.make_async_copy(src, src, store_sem.at[job]).wait()


def place_grads(fin, y, gain_sum):
    any_spec = pl.BlockSpec(memory_space=pl.ANY)
    shard = jax.ShapeDtypeStruct((LAYERS, GR, FF), F32)
    dma = pltpu.SemaphoreType.DMA
    return pl.pallas_call(
        place_kernel,
        in_specs=[any_spec, any_spec, pl.BlockSpec(memory_space=pltpu.VMEM)],
        out_specs=[*[any_spec] * 4, pl.BlockSpec(memory_space=pltpu.VMEM)],
        out_shape=[shard, shard, jax.ShapeDtypeStruct((LAYERS, D, D), F32), jax.ShapeDtypeStruct((TOK, D), BF16),
                   jax.ShapeDtypeStruct((LAYERS, D), F32)],
        scratch_shapes=[pltpu.VMEM((JOBS, *BLK), F32), pltpu.VMEM((TOK, D), BF16), dma((JOBS,)), dma((JOBS,)),
                        dma((NT,)), dma((NT,))],
        compiler_params=pltpu.CompilerParams(vmem_limit_bytes=VMEM_MAX),
        cost_estimate=pl.CostEstimate(flops=0, bytes_accessed=41 << 20, transcendentals=0),
        name="place_grads",
    )(fin, y, gain_sum)


def solution(mesh):
    tok_spec = P(TOKEN_AXES, None)
    shard_spec = P(None, "fsdp", None)
    full_spec = P(None, None)

    def device_step(x_local, dy_local, w_gate_sh, w_up_sh, w_down_sh, norm_gain):
        gu0, h1, wgu, wd = forward_gather(x_local, norm_gain, w_gate_sh, w_up_sh, w_down_sh)
        y_local, _, _, fin, gain_sum = backward_reduce(h1, x_local, norm_gain, wgu, wd, gu0, dy_local)
        d_gate, d_up, d_down, y_out, d_gain = place_grads(fin, y_local, gain_sum)
        return y_out, d_gate, d_up, d_down, d_gain

    return jax.shard_map(device_step, mesh=mesh,
                         in_specs=(tok_spec, tok_spec, shard_spec, shard_spec, shard_spec, full_spec),
                         out_specs=(tok_spec, shard_spec, shard_spec, shard_spec, full_spec), check_vma=False)
```
